1024 devices in a mesh: ta: 32 (over z, x_lo), gz: 4 (over x_hi, core), gy: 8 (over y).
Axes of the slice: x: 4 (x_hi: 2, x_lo: 2; x = x_hi * 2 + x_lo), y: 8, z: 16, core: 2. Of those that a mesh axis runs over, the one named last changes fastest.
Arguments:
- source: float32 [2, 4, 3, 128, 16, 1024], P(None, None, None, 'ta', 'gz', 'gy'), may hold values from -6 to 6
- start_guess: float32 [2, 4, 3, 128, 16, 1024], P(None, None, None, 'ta', 'gz', 'gy'), may hold values from -3 to 3
- gauge_links: float32 [4, 2, 3, 3, 128, 16, 1024], P(None, None, None, None, 'ta', 'gz', 'gy'), may hold values from -1 to 1, as said below
- clover: float32 [2, 2, 6, 6, 128, 16, 1024], P(None, None, None, None, 'ta', 'gz', 'gy'), may hold values from -1.5 to 5.9, as said below
Outputs:
- update: float32 [2, 4, 3, 128, 16, 1024], P(None, None, None, 'ta', 'gz', 'gy')
- profile: float32 [128], P('ta')
The draws below stay inside these ranges and needn't reach their ends.
Inputs may be any that keep to these rules, and one draw needn't show every extreme that they name: `gauge_links`: every link is a special unitary 3x3 matrix. `clover`: each chiral block is Hermitian.
All inputs are finite; a program needn't handle non-finite values.
Results may differ from the reference program's by a relative error of at most 0.0003.
Values sent between devices are 32-bit elements; how exact they have to be, the bound alone decides.
No kernel may reach another device: no remote copies, remote signals or barrier semaphores. Data moves between devices by JAX's collectives and lax.ppermute only.
A program may use at most 64 MiB of HBM per device.

```python
import jax
import jax.numpy as jnp
import numpy as np
from jax import lax

LX = 32
BLOCK = 4
MR_STEPS = 4
NT = 128
NZ = 16
NY = 32
NX = 32


def normalise(vec_re, vec_im):
    inverse_norm = lax.rsqrt(jnp.sum(vec_re * vec_re + vec_im * vec_im, axis=1, keepdims=True))
    return (vec_re * inverse_norm, vec_im * inverse_norm)


def draw_gauge_links(key, part):
    raw_draw = jax.random.normal(jax.random.fold_in(key, 11), (4, 2, 2, 3, NT, NZ, NY * NX), jnp.float32)
    first_re, first_im = normalise(raw_draw[:, 0, 0], raw_draw[:, 0, 1])
    other_re = raw_draw[:, 1, 0]
    other_im = raw_draw[:, 1, 1]
    inner_re = jnp.sum(first_re * other_re + first_im * other_im, axis=1, keepdims=True)
    inner_im = jnp.sum(first_re * other_im - first_im * other_re, axis=1, keepdims=True)
    second_re, second_im = normalise(other_re - (inner_re * first_re - inner_im * first_im), other_im - (inner_re * first_im + inner_im * first_re))
    third_re = []
    third_im = []
    for colour_index in range(3):
        next_one = (colour_index + 1) % 3
        next_two = (colour_index + 2) % 3
        cross_re = first_re[:, next_one] * second_re[:, next_two] - first_im[:, next_one] * second_im[:, next_two] - (first_re[:, next_two] * second_re[:, next_one] - first_im[:, next_two] * second_im[:, next_one])
        cross_im = first_re[:, next_one] * second_im[:, next_two] + first_im[:, next_one] * second_re[:, next_two] - (first_re[:, next_two] * second_im[:, next_one] + first_im[:, next_two] * second_re[:, next_one])
        third_re.append(cross_re)
        third_im.append(-cross_im)
    link_re = jnp.stack([first_re, second_re, jnp.stack(third_re, axis=1)], axis=1)
    link_im = jnp.stack([first_im, second_im, jnp.stack(third_im, axis=1)], axis=1)
    return jnp.stack([link_re, link_im], axis=1)


def draw_clover(key, part):
    full_shape = (2, 2, 6, 6, NT, NZ, NY * NX)
    raw_draw = jnp.clip(0.3 * jax.random.normal(jax.random.fold_in(key, 23), full_shape, jnp.float32), -1.5, 1.5)
    herm_re = 0.5 * (raw_draw[:, 0] + jnp.swapaxes(raw_draw[:, 0], 1, 2))
    herm_im = 0.5 * (raw_draw[:, 1] - jnp.swapaxes(raw_draw[:, 1], 1, 2))
    diagonal = 4.4 * jnp.eye(6, dtype=jnp.float32)[None, :, :, None, None, None]
    return jnp.stack([herm_re + diagonal, herm_im], axis=1)


def shard_levels(own_key, shape, shards, least, high):
    def one(axis_at, blocks):
        steps = jax.random.uniform(jax.random.fold_in(jax.random.fold_in(own_key, 6), axis_at), (blocks,), jnp.float32, least / len(shards), high / len(shards))
        return jnp.repeat(jnp.exp(steps), shape[axis_at] // blocks).reshape((-1,) + (1,) * (len(shape) - axis_at - 1))

    loudness = one(*shards[0])
    for cut in shards[1:]:
        loudness = loudness * one(*cut)
    return loudness


def gaussian(stream_key, extent, spread, bound, cuts=(), held_as=jnp.bfloat16):
    values = jax.random.normal(stream_key, extent, jnp.float32) * spread
    if len(cuts) > 0:
        values = shard_levels(stream_key, extent, cuts, -0.22, 0.18) * values
    return jnp.clip(values, min=-bound, max=bound).astype(held_as)


def setup_inputs(seed: int = 0) -> dict:
    key_of = jax.random.split(jax.random.key(seed), 5)
    return {
        "source": gaussian(key_of[0], (2, 4, 3, NT, NZ, NY * NX), 1.0, 6.0, ((3, 32), (4, 4), (5, 8)), jnp.float32),
        "start_guess": gaussian(key_of[1], (2, 4, 3, NT, NZ, NY * NX), 0.5, 3.0, ((3, 32), (4, 4), (5, 8)), jnp.float32),
        "gauge_links": draw_gauge_links(jax.random.fold_in(key_of[4], 71), 0),
        "clover": draw_clover(jax.random.fold_in(key_of[4], 71), 0),
    }


EPSILON = 1e-6


def upper_pair(direction):
    if direction == 0:
        return np.eye(2), np.zeros((2, 2))
    if direction == 1:
        return np.zeros((2, 2)), -np.array([[1.0, 0.0], [0.0, -1.0]])
    if direction == 2:
        return np.array([[0.0, -1.0], [1.0, 0.0]]), np.zeros((2, 2))
    return np.zeros((2, 2)), -np.array([[0.0, 1.0], [1.0, 0.0]])


def hop_table(direction, sign_flip):
    upper_re, upper_im = upper_pair(direction)
    table_re = np.eye(4)
    table_im = np.zeros((4, 4))
    table_re[:2, 2:] = sign_flip * upper_re
    table_im[:2, 2:] = sign_flip * upper_im
    table_re[2:, :2] = sign_flip * upper_re.T
    table_im[2:, :2] = -sign_flip * upper_im.T
    return table_re, table_im


def spin_apply(spin_tables, spinor):
    table_re, table_im = spin_tables
    re_rows = []
    im_rows = []
    for row_index in range(table_re.shape[0]):
        result_re = jnp.zeros_like(spinor[0, 0])
        result_im = jnp.zeros_like(spinor[0, 0])
        for col_index in range(table_re.shape[1]):
            coef_re = float(table_re[row_index, col_index])
            coef_im = float(table_im[row_index, col_index])
            if coef_re != 0.0:
                result_re = result_re + coef_re * spinor[0, col_index]
                result_im = result_im + coef_re * spinor[1, col_index]
            if coef_im != 0.0:
                result_re = result_re - coef_im * spinor[1, col_index]
                result_im = result_im + coef_im * spinor[0, col_index]
        re_rows.append(result_re)
        im_rows.append(result_im)
    return jnp.stack([jnp.stack(re_rows), jnp.stack(im_rows)])


def colour_apply(gauge_link, spinor):
    result_re = jnp.zeros((spinor.shape[1],) + gauge_link.shape[1:2] + spinor.shape[3:], spinor.dtype)
    result_im = jnp.zeros_like(result_re)
    for col_index in range(3):
        link_re = gauge_link[0, :, col_index][None]
        link_im = gauge_link[1, :, col_index][None]
        vec_re = spinor[0, :, col_index][:, None]
        vec_im = spinor[1, :, col_index][:, None]
        result_re = result_re + link_re * vec_re - link_im * vec_im
        result_im = result_im + link_re * vec_im + link_im * vec_re
    return jnp.stack([result_re, result_im])


def colour_adjoint(gauge_link, spinor):
    result_re = jnp.zeros((spinor.shape[1],) + gauge_link.shape[1:2] + spinor.shape[3:], spinor.dtype)
    result_im = jnp.zeros_like(result_re)
    for col_index in range(3):
        link_re = gauge_link[0, col_index, :][None]
        link_im = gauge_link[1, col_index, :][None]
        vec_re = spinor[0, :, col_index][:, None]
        vec_im = spinor[1, :, col_index][:, None]
        result_re = result_re + link_re * vec_re + link_im * vec_im
        result_im = result_im + link_re * vec_im - link_im * vec_re
    return jnp.stack([result_re, result_im])


def site_apply(clover, spinor):
    halves = spinor.reshape((2, 2, 6) + spinor.shape[3:])
    result_re = jnp.zeros(halves.shape[1:], spinor.dtype)
    result_im = jnp.zeros_like(result_re)
    for col_index in range(6):
        matrix_re = clover[:, 0, :, col_index]
        matrix_im = clover[:, 1, :, col_index]
        vec_re = halves[0][:, col_index][:, None]
        vec_im = halves[1][:, col_index][:, None]
        result_re = result_re + matrix_re * vec_re - matrix_im * vec_im
        result_im = result_im + matrix_re * vec_im + matrix_im * vec_re
    return jnp.stack([result_re, result_im]).reshape(spinor.shape)


def local_neighbour(spinor, direction, offset):
    if direction == 0:
        return jnp.roll(spinor, -offset, axis=3)
    if direction == 1:
        return jnp.roll(spinor, -offset, axis=4)
    if direction == 2:
        return jnp.roll(spinor, -offset * LX, axis=5)
    shifted = jnp.roll(spinor, -offset, axis=5)
    wrapped = jnp.roll(spinor, offset * (LX - 1), axis=5)
    position = jnp.arange(spinor.shape[5]) % LX
    edge_index = LX - 1 if offset > 0 else 0
    return jnp.where(position == edge_index, wrapped, shifted)


def lattice_neighbour(spinor, direction, offset):
    rolled = local_neighbour(spinor, direction, offset)
    if direction != 0:
        return rolled
    edge_index = NT - 1 if offset > 0 else 0
    sign_flip = jnp.where(jnp.arange(NT) == edge_index, -1.0, 1.0).astype(jnp.float32)
    return rolled * sign_flip[:, None, None]


def block_mask(site_shape, direction, offset):
    if direction == 0:
        coordinate = jnp.arange(site_shape[0])[:, None, None]
    elif direction == 1:
        coordinate = jnp.arange(site_shape[1])[None, :, None]
    elif direction == 2:
        coordinate = (jnp.arange(site_shape[2]) // LX)[None, None, :]
    else:
        coordinate = (jnp.arange(site_shape[2]) % LX)[None, None, :]
    position = coordinate % BLOCK
    edge_index = BLOCK - 1 if offset > 0 else 0
    return (position != edge_index).astype(jnp.float32)


def apply_operator(spinor, gauge_links, clover, neighbour, masked):
    summed = site_apply(clover, spinor)
    site_shape = spinor.shape[3:]
    for direction in range(4):
        gauge_link = gauge_links[direction]
        forward = spin_apply(hop_table(direction, -1.0), colour_apply(gauge_link, neighbour(spinor, direction, 1)))
        behind = spin_apply(hop_table(direction, 1.0), neighbour(colour_adjoint(gauge_link, spinor), direction, -1))
        if masked:
            forward = forward * block_mask(site_shape, direction, 1)
            behind = behind * block_mask(site_shape, direction, -1)
        summed = summed - 0.5 * (forward + behind)
    return summed


def block_spread(site_values):
    time_len, depth_len, flat_len = site_values.shape
    rows_len = flat_len // LX
    blocked = site_values.reshape((time_len // BLOCK, BLOCK, depth_len // BLOCK, BLOCK, rows_len // BLOCK, BLOCK, LX // BLOCK, BLOCK))
    totals = jnp.sum(blocked, axis=(1, 3, 5, 7), keepdims=True)
    return jnp.broadcast_to(totals, blocked.shape).reshape(site_values.shape)


def minimal_residual(initial_residual, gauge_links, clover):
    correction = jnp.zeros_like(initial_residual)
    remainder = initial_residual
    for repeat in range(MR_STEPS):
        applied = apply_operator(remainder, gauge_links, clover, local_neighbour, True)
        margin_re = block_spread(jnp.sum(applied[0] * remainder[0] + applied[1] * remainder[1], axis=(0, 1)))
        margin_im = block_spread(jnp.sum(applied[0] * remainder[1] - applied[1] * remainder[0], axis=(0, 1)))
        norm_sq = block_spread(jnp.sum(applied * applied, axis=(0, 1, 2))) + EPSILON
        alpha_re = margin_re / norm_sq
        alpha_im = margin_im / norm_sq
        correction = correction + jnp.stack([alpha_re * remainder[0] - alpha_im * remainder[1], alpha_re * remainder[1] + alpha_im * remainder[0]])
        remainder = remainder - jnp.stack([alpha_re * applied[0] - alpha_im * applied[1], alpha_re * applied[1] + alpha_im * applied[0]])
    return correction, remainder


def reference(source, start_guess, gauge_links, clover):
    initial_residual = source - apply_operator(start_guess, gauge_links, clover, lattice_neighbour, False)
    correction, remainder = minimal_residual(initial_residual, gauge_links, clover)
    update = start_guess + correction
    latest = source - apply_operator(update, gauge_links, clover, lattice_neighbour, False)
    profile = jnp.sum(latest * latest, axis=(0, 1, 2, 4, 5)) / jnp.sum(source * source, axis=(0, 1, 2, 4, 5))
    return update, profile
```

```python
import jax
import jax.numpy as jnp
from jax import lax
from jax.experimental import pallas as pl
from jax.experimental.pallas import tpu as pltpu
from jax.sharding import Mesh
from jax.sharding import PartitionSpec as P

LX = 32
MR_STEPS = 4
EPSILON = 1e-06
GZ = ("gz_0", "gz_1")
ROWS, LANES = 16, 128
AXES = ("ta", GZ, "gy")
MESSAGES = ((0, 1), (0, 0), (2, 1), (2, 0), (1, 1), (1, 0))

UPPER = (
    ((0, 1), (1, 1)),
    ((0, -1j), (1, 1j)),
    ((1, -1), (0, 1)),
    ((1, -1j), (0, -1j)),
)


def times(coef, value):
    re, im = value
    if coef == 1:
        return re, im
    if coef == -1:
        return -re, -im
    if coef == 1j:
        return -im, re
    return im, -re


def plus(a, b):
    return a[0] + b[0], a[1] + b[1]


def plus_times(a, coef, b):
    if coef == 1:
        return a[0] + b[0], a[1] + b[1]
    if coef == -1:
        return a[0] - b[0], a[1] - b[1]
    if coef == 1j:
        return a[0] - b[1], a[1] + b[0]
    return a[0] + b[1], a[1] - b[0]


def iota(axis):
    return lax.broadcasted_iota(jnp.int32, (ROWS, LANES), axis)


def roll(value, shift, axis):
    size = value.shape[axis]
    shift = shift % size
    if shift == 0:
        return value
    return pltpu.roll(value, shift, axis)


def spinor_at(ref, spin, colour, rows=slice(None)):
    return ref[3 * spin + colour, rows], ref[12 + 3 * spin + colour, rows]


def half_spinor(ref, direction, row, sign, rows=slice(None)):
    column, entry = UPPER[direction][row]
    return [
        plus_times(spinor_at(ref, row, colour, rows), sign * entry, spinor_at(ref, 2 + column, colour, rows))
        for colour in range(3)
    ]


def link_at(links, direction, row, column, rows=slice(None)):
    base = 18 * direction + 3 * row + column
    return links[base, rows], links[base + 9, rows]


def link_times(links, direction, vector, rows=slice(None)):
    out = []
    for row in range(3):
        re = im = None
        for column in range(3):
            u_re, u_im = link_at(links, direction, row, column, rows)
            v_re, v_im = vector[column]
            t_re, t_im = u_re * v_re - u_im * v_im, u_re * v_im + u_im * v_re
            re, im = (t_re, t_im) if re is None else (re + t_re, im + t_im)
        out.append((re, im))
    return out


def link_adjoint_times(links, direction, vector, rows=slice(None)):
    out = []
    for row in range(3):
        re = im = None
        for column in range(3):
            u_re, u_im = link_at(links, direction, column, row, rows)
            v_re, v_im = vector[column]
            t_re, t_im = u_re * v_re + u_im * v_im, u_re * v_im - u_im * v_re
            re, im = (t_re, t_im) if re is None else (re + t_re, im + t_im)
        out.append((re, im))
    return out


def add_hops(out_ref, direction, row, forward, behind, sign=1):
    column, entry = UPPER[direction][row]
    conj = complex(entry).conjugate()
    for colour in range(3):
        upper = plus(forward[colour], behind[colour])
        lower = times(conj, plus_times(behind[colour], -1, forward[colour]))
        for spin, value in ((row, upper), (2 + column, lower)):
            k = 3 * spin + colour
            out_ref[k] = out_ref[k] + value[0]
            out_ref[12 + k] = out_ref[12 + k] + value[1]


def shift(value, direction, offset, periodic):
    if direction == 0:
        return roll(value, -4 * offset, 0)
    if direction == 1:
        return roll(value, -offset, 0)
    if direction == 2:
        return roll(value, -LX * offset, 1)
    near = roll(value, -offset, 1)
    if not periodic:
        return near
    edge = (LX - 1) if offset > 0 else 0
    return jnp.where(iota(1) % LX == edge, roll(value, offset * (LX - 1), 1), near)


def inside(direction, offset):
    edge = 3 if offset > 0 else 0
    if direction == 0:
        return iota(0) // 4 != edge
    if direction == 1:
        return iota(0) % 4 != edge
    if direction == 2:
        return iota(1) // LX != edge
    return iota(1) % 4 != edge


def site_terms(out_ref, clover, ref, add=False):
    for chirality in range(2):
        for a in range(6):
            re = im = None
            for b in range(6):
                base = 72 * chirality + 6 * a + b
                m_re, m_im = clover[base], clover[base + 36]
                v_re, v_im = ref[6 * chirality + b], ref[12 + 6 * chirality + b]
                t_re, t_im = m_re * v_re - m_im * v_im, m_re * v_im + m_im * v_re
                re, im = (t_re, t_im) if re is None else (re + t_re, im + t_im)
            k = 6 * chirality + a
            out_ref[k] = out_ref[k] + re if add else re
            out_ref[12 + k] = out_ref[12 + k] + im if add else im


def hop_terms(out_ref, links, ref, direction, weight_ahead, weight_behind, periodic):
    for row in range(2):
        ahead = half_spinor(ref, direction, row, -1)
        ahead = [tuple(shift(p, direction, 1, periodic) * weight_ahead for p in c) for c in ahead]
        forward = link_times(links, direction, ahead)
        behind = link_adjoint_times(links, direction, half_spinor(ref, direction, row, 1))
        behind = [tuple(shift(p, direction, -1, periodic) * weight_behind for p in c) for c in behind]
        add_hops(out_ref, direction, row, forward, behind)


def weights(direction, scale, outside=False):
    pair = []
    for offset in (1, -1):
        keep = inside(direction, offset)
        pair.append(jnp.where(keep, 0.0, scale) if outside else jnp.where(keep, scale, 0.0))
    return pair


def block_hops(out_ref, links, ref, weight_ref, x_periodic):
    for direction in range(4):
        if direction == 3 and x_periodic:
            hop_terms(out_ref, links, ref, 3, jnp.float32(-0.5), jnp.float32(-0.5), True)
        else:
            hop_terms(out_ref, links, ref, direction, weight_ref[2 * direction], weight_ref[2 * direction + 1], False)


def fill_weights(weight_ref):
    for direction in range(4):
        ahead, behind = weights(direction, -0.5)
        weight_ref[2 * direction] = ahead
        weight_ref[2 * direction + 1] = behind


def packed(vectors, direction, edge):
    flat = [part for vector in vectors for colour in vector for part in colour]
    tiles = []
    for group in range(3):
        tile = None
        for j in range(4):
            value = flat[4 * group + j]
            if direction == 0:
                moved, keep = roll(value, 4 * (j - edge), 0), iota(0) // 4 == j
            elif direction == 1:
                moved, keep = roll(value, j - edge, 0), iota(0) % 4 == j
            else:
                moved, keep = roll(value, LX * (j - edge), 1), iota(1) // LX == j
            tile = moved if tile is None else jnp.where(keep, moved, tile)
        tiles.append(tile)
    return tiles


def unpacked(tiles, direction, edge, scale):
    if direction == 0:
        weight = jnp.where(iota(0) // 4 == edge, scale, 0.0)
    elif direction == 1:
        weight = jnp.where(iota(0) % 4 == edge, scale, 0.0)
    else:
        weight = jnp.where(iota(1) // LX == edge, scale, 0.0)
    flat = []
    for group in range(3):
        for j in range(4):
            if direction == 0:
                moved = roll(tiles[group], 4 * (edge - j), 0)
            elif direction == 1:
                moved = roll(tiles[group], edge - j, 0)
            else:
                moved = roll(tiles[group], LX * (edge - j), 1)
            flat.append(moved * weight)
    pairs = [(flat[2 * k], flat[2 * k + 1]) for k in range(6)]
    return pairs[:3], pairs[3:]


def write_faces(face_refs, ref, links):
    for direction in range(3):
        up = packed(
            [link_adjoint_times(links, direction, half_spinor(ref, direction, row, 1)) for row in range(2)],
            direction, 3)
        down = packed([half_spinor(ref, direction, row, -1) for row in range(2)], direction, 0)
        even = lax.axis_index(AXES[direction]) % 2 == 0
        for group in range(3):
            rows = pl.ds(ROWS * group, ROWS)
            face_refs[MESSAGES.index((direction, 0))][rows] = jnp.where(even, up[group], down[group])
            face_refs[MESSAGES.index((direction, 1))][rows] = jnp.where(even, down[group], up[group])


def halo_hops(out_ref, links, face_refs):
    for direction in range(3):
        even = lax.axis_index(AXES[direction]) % 2 == 0
        above, below = [], []
        for group in range(3):
            rows = pl.ds(ROWS * group, ROWS)
            first, second = (face_refs[MESSAGES.index((direction, k))][rows] for k in range(2))
            above.append(jnp.where(even, first, second))
            below.append(jnp.where(even, second, first))
        scale_above = scale_below = jnp.float32(0.5)
        if direction == 0:
            place, last = lax.axis_index("ta"), lax.axis_size("ta") - 1
            scale_above = jnp.where(place == last, jnp.float32(-0.5), jnp.float32(0.5))
            scale_below = jnp.where(place == 0, jnp.float32(-0.5), jnp.float32(0.5))
        ahead = unpacked(above, direction, 3, scale_above)
        behind = unpacked(below, direction, 0, scale_below)
        for row in range(2):
            add_hops(out_ref, direction, row, link_times(links, direction, ahead[row]), behind[row])


def block_total(value):
    total = value[:8] + value[8:]
    for step in (4, 2, 1):
        total = total + roll(total, step, 0)
    for step in (2 * LX, LX):
        total = total + roll(total, step, 1)
    lane = lax.broadcasted_iota(jnp.int32, (8, LANES), 1)
    for step in (1, 2):
        total = total + jnp.where((lane // step) % 2 == 0, roll(total, -step, 1), roll(total, step, 1))
    return total


def send_kernel(start_hbm, links_hbm, start, links, *rest):
    faces, sems = rest[:6], rest[6]
    near, far = pl.ds(0, 54), pl.ds(54, 18)
    copies = [
        pltpu.make_async_copy(start_hbm, start, sems.at[0]),
        pltpu.make_async_copy(links_hbm.at[near], links.at[near], sems.at[1]),
        pltpu.make_async_copy(links_hbm.at[far], links.at[far], sems.at[2]),
    ]
    for copy in copies:
        copy.start()
    copies[0].wait()
    copies[1].wait()
    write_faces(faces, start, links)
    copies[2].wait()


def residual_kernel(source_hbm, clover_hbm, start, links, partial, clover, source_sq, source, weight_ref, sems):
    copies = [
        pltpu.make_async_copy(clover_hbm, clover, sems.at[0]),
        pltpu.make_async_copy(source_hbm, source, sems.at[1]),
    ]
    for copy in copies:
        copy.start()
    fill_weights(weight_ref)
    for k in range(24):
        partial[k] = jnp.zeros((ROWS, LANES), jnp.float32)
    block_hops(partial, links, start, weight_ref, True)
    copies[0].wait()
    site_terms(partial, clover, start, True)
    copies[1].wait()
    total = None
    for k in range(24):
        value = source[k]
        partial[k] = value - partial[k]
        total = value * value if total is None else total + value * value
    source_sq[...] = total


def sweep_kernel(partial, links, clover, *rest):
    received, sent = rest[:6], rest[6:12]
    correction, remainder, applied, weight_ref = rest[12:]
    fill_weights(weight_ref)
    for k in range(24):
        remainder[k] = partial[k]
        correction[k] = jnp.zeros((ROWS, LANES), jnp.float32)
    halo_hops(remainder, links, received)

    def step(_, carry):
        site_terms(applied, clover, remainder)
        block_hops(applied, links, remainder, weight_ref, False)
        dot_re = dot_im = norm = None
        for k in range(12):
            a_re, a_im, r_re, r_im = applied[k], applied[12 + k], remainder[k], remainder[12 + k]
            terms = (a_re * r_re + a_im * r_im, a_re * r_im - a_im * r_re, a_re * a_re + a_im * a_im)
            dot_re, dot_im, norm = terms if k == 0 else (dot_re + terms[0], dot_im + terms[1], norm + terms[2])
        norm = block_total(norm) + EPSILON
        alpha_re, alpha_im = block_total(dot_re) / norm, block_total(dot_im) / norm
        alpha_re = jnp.concatenate([alpha_re, alpha_re], axis=0)
        alpha_im = jnp.concatenate([alpha_im, alpha_im], axis=0)
        for k in range(12):
            a_re, a_im, r_re, r_im = applied[k], applied[12 + k], remainder[k], remainder[12 + k]
            correction[k] = correction[k] + (alpha_re * r_re - alpha_im * r_im)
            correction[12 + k] = correction[12 + k] + (alpha_re * r_im + alpha_im * r_re)
            remainder[k] = r_re - (alpha_re * a_re - alpha_im * a_im)
            remainder[12 + k] = r_im - (alpha_re * a_im + alpha_im * a_re)
        return carry

    lax.fori_loop(0, MR_STEPS, step, 0)
    write_faces(sent, correction, links)


def inner_kernel(start, correction, remainder, links, update_hbm, latest, update, sem):
    for k in range(24):
        update[k] = start[k] + correction[k]
        latest[k] = remainder[k]
    copy = pltpu.make_async_copy(update, update_hbm, sem)
    copy.start()
    ahead, behind = weights(3, 0.5, outside=True)
    hop_terms(latest, links, correction, 3, ahead, behind, True)
    copy.wait()


def latest_kernel(partial, source_sq, links, *rest):
    received, sums, latest = rest[:6], rest[6], rest[7]
    for k in range(24):
        latest[k] = partial[k]
    halo_hops(latest, links, received)
    total = None
    for k in range(24):
        square = latest[k] * latest[k]
        total = square if total is None else total + square
    slices = [
        jnp.sum(value[4 * t:4 * t + 4], axis=0, keepdims=True)
        for value in (total, source_sq[...]) for t in range(4)
    ]
    slices = jnp.concatenate(slices, axis=0)
    for k in range(sums.shape[0]):
        sums[k] = slices


PARAMS = pltpu.CompilerParams(vmem_limit_bytes=12 * 2**20)
FIELD = pltpu.VMEM((24, ROWS, LANES), jnp.float32)
FACE = pltpu.VMEM((48, LANES), jnp.float32)
SCRATCH = pltpu.VMEM((24, ROWS, LANES), jnp.float32)
IN_HBM = pl.BlockSpec(memory_space=pltpu.HBM)
WEIGHTS = pltpu.VMEM((8, ROWS, LANES), jnp.float32)


def in_vmem(value):
    return pltpu.with_memory_space_constraint(value, pltpu.VMEM)


def in_hbm(value):
    return pltpu.with_memory_space_constraint(value, pltpu.HBM)


def call(body, outs, scratch=(), flops=10_000_000):
    kernel = pl.pallas_call(
        body,
        out_shape=outs,
        scratch_shapes=scratch,
        compiler_params=PARAMS,
        cost_estimate=pl.CostEstimate(flops=flops, transcendentals=0, bytes_accessed=2_000_000),
    )
    return lambda *args: kernel(*map(in_vmem, args))


def matching(count, first):
    pairs = []
    for low in range(first, count + first, 2):
        a, b = low % count, (low + 1) % count
        pairs += [(a, b), (b, a)]
    return pairs


def exchange(faces):
    received = []
    for face, (direction, first) in zip(faces, MESSAGES):
        axis = AXES[direction]
        received.append(lax.ppermute(face, axis, matching(lax.axis_size(axis), first)))
    return received


def local(source, start_guess, gauge_links, clover):
    shape = source.shape
    source = source.reshape(24, ROWS, LANES)
    start = start_guess.reshape(24, ROWS, LANES)
    links = gauge_links.reshape(72, ROWS, LANES)
    clover = clover.reshape(144, ROWS, LANES)
    start, links, *faces = pl.pallas_call(
        send_kernel,
        in_specs=[IN_HBM] * 2,
        out_shape=[FIELD, pltpu.VMEM(links.shape, jnp.float32)] + [FACE] * 6,
        scratch_shapes=[pltpu.SemaphoreType.DMA((3,))],
        compiler_params=PARAMS,
    )(in_hbm(start), in_hbm(links))
    received = exchange(faces)
    partial, clover, source_sq = pl.pallas_call(
        residual_kernel,
        in_specs=[IN_HBM] * 2 + [pl.BlockSpec(memory_space=pltpu.VMEM)] * 2,
        out_shape=[FIELD, pltpu.VMEM(clover.shape, jnp.float32), pltpu.VMEM((ROWS, LANES), jnp.float32)],
        scratch_shapes=[SCRATCH, WEIGHTS, pltpu.SemaphoreType.DMA((2,))],
        compiler_params=PARAMS,
        cost_estimate=pl.CostEstimate(flops=10_000_000, transcendentals=0, bytes_accessed=2_000_000),
    )(in_hbm(source), in_hbm(clover), in_vmem(start), in_vmem(links))
    *faces, correction, remainder = call(sweep_kernel, [FACE] * 6 + [FIELD] * 2, [SCRATCH, WEIGHTS])(
        partial, links, clover, *received)
    received = exchange(faces)
    update, latest = call(
        inner_kernel, [pltpu.HBM(source.shape, jnp.float32), FIELD], [SCRATCH, pltpu.SemaphoreType.DMA(())])(
            start, correction, remainder, links)
    group = GZ + ("gy",)
    sums = call(latest_kernel, pltpu.VMEM((lax.axis_size(group), 8, LANES), jnp.float32), [SCRATCH])(
        latest, source_sq, links, *received)
    sums = lax.all_to_all(sums, group, 0, 0)
    sums = jnp.sum(sums, axis=(0, 2))
    return update.reshape(shape), sums[:4] / sums[4:]


def solution(mesh):
    finer = Mesh(
        mesh.devices.reshape(mesh.shape["ta"], 2, 2, mesh.shape["gy"]), ("ta", "gz_0", "gz_1", "gy")
    )
    field = P(None, None, None, "ta", GZ, "gy")
    matrix = P(None, None, None, None, "ta", GZ, "gy")
    return jax.shard_map(
        local, mesh=finer, in_specs=(field, field, matrix, matrix), out_specs=(field, P("ta")), check_vma=False
    )
```

```python
import jax
import jax.numpy as jnp
from jax import lax
from jax.experimental import pallas as pl
from jax.experimental.pallas import tpu as pltpu
from jax.sharding import Mesh
from jax.sharding import PartitionSpec as P

LX = 32
MR_STEPS = 4
EPSILON = 1e-06
GZ = ("gz_0", "gz_1")
ROWS, LANES = 16, 128
AXES = ("ta", GZ, "gy")
MESSAGES = ((0, 1), (0, 0), (2, 1), (2, 0), (1, 1), (1, 0))

UPPER = (
    ((0, 1), (1, 1)),
    ((0, -1j), (1, 1j)),
    ((1, -1), (0, 1)),
    ((1, -1j), (0, -1j)),
)


def times(coef, value):
    re, im = value
    if coef == 1:
        return re, im
    if coef == -1:
        return -re, -im
    if coef == 1j:
        return -im, re
    return im, -re


def plus(a, b):
    return a[0] + b[0], a[1] + b[1]


def plus_times(a, coef, b):
    if coef == 1:
        return a[0] + b[0], a[1] + b[1]
    if coef == -1:
        return a[0] - b[0], a[1] - b[1]
    if coef == 1j:
        return a[0] - b[1], a[1] + b[0]
    return a[0] + b[1], a[1] - b[0]


def iota(axis):
    return lax.broadcasted_iota(jnp.int32, (ROWS, LANES), axis)


def roll(value, shift, axis):
    size = value.shape[axis]
    shift = shift % size
    if shift == 0:
        return value
    return pltpu.roll(value, shift, axis)


def spinor_at(ref, spin, colour, rows=slice(None)):
    return ref[3 * spin + colour, rows], ref[12 + 3 * spin + colour, rows]


def half_spinor(ref, direction, row, sign, rows=slice(None)):
    column, entry = UPPER[direction][row]
    return [
        plus_times(spinor_at(ref, row, colour, rows), sign * entry, spinor_at(ref, 2 + column, colour, rows))
        for colour in range(3)
    ]


def link_at(links, direction, row, column, rows=slice(None)):
    base = 18 * direction + 3 * row + column
    return links[base, rows], links[base + 9, rows]


def link_times(links, direction, vector, rows=slice(None)):
    out = []
    for row in range(3):
        re = im = None
        for column in range(3):
            u_re, u_im = link_at(links, direction, row, column, rows)
            v_re, v_im = vector[column]
            t_re, t_im = u_re * v_re - u_im * v_im, u_re * v_im + u_im * v_re
            re, im = (t_re, t_im) if re is None else (re + t_re, im + t_im)
        out.append((re, im))
    return out


def link_adjoint_times(links, direction, vector, rows=slice(None)):
    out = []
    for row in range(3):
        re = im = None
        for column in range(3):
            u_re, u_im = link_at(links, direction, column, row, rows)
            v_re, v_im = vector[column]
            t_re, t_im = u_re * v_re + u_im * v_im, u_re * v_im - u_im * v_re
            re, im = (t_re, t_im) if re is None else (re + t_re, im + t_im)
        out.append((re, im))
    return out


def add_hops(out_ref, direction, row, forward, behind, sign=1):
    column, entry = UPPER[direction][row]
    conj = complex(entry).conjugate()
    for colour in range(3):
        upper = plus(forward[colour], behind[colour])
        lower = times(conj, plus_times(behind[colour], -1, forward[colour]))
        for spin, value in ((row, upper), (2 + column, lower)):
            k = 3 * spin + colour
            out_ref[k] = out_ref[k] + value[0]
            out_ref[12 + k] = out_ref[12 + k] + value[1]


def shift(value, direction, offset, periodic):
    if direction == 0:
        low, high = roll(value[:8], 4, 0), roll(value[8:], 4, 0)
        front = lax.broadcasted_iota(jnp.int32, (8, LANES), 0) < 4
        if offset > 0:
            return jnp.concatenate([jnp.where(front, low, high), high], axis=0)
        return jnp.concatenate([low, jnp.where(front, low, high)], axis=0)
    if direction == 1:
        return jnp.concatenate([roll(value[:8], -offset, 0), roll(value[8:], -offset, 0)], axis=0)
    if direction == 2:
        return roll(value, -LX * offset, 1)
    near = roll(value, -offset, 1)
    if not periodic:
        return near
    edge = (LX - 1) if offset > 0 else 0
    return jnp.where(iota(1) % LX == edge, roll(value, offset * (LX - 1), 1), near)


def inside(direction, offset):
    edge = 3 if offset > 0 else 0
    if direction == 0:
        return iota(0) // 4 != edge
    if direction == 1:
        return iota(0) % 4 != edge
    if direction == 2:
        return iota(1) // LX != edge
    return iota(1) % 4 != edge


def site_terms(out_ref, clover, ref, add=False):
    for chirality in range(2):
        for a in range(6):
            re = im = None
            for b in range(6):
                base = 72 * chirality + 6 * a + b
                m_re, m_im = clover[base], clover[base + 36]
                v_re, v_im = ref[6 * chirality + b], ref[12 + 6 * chirality + b]
                if a == b:
                    t_re, t_im = m_re * v_re, m_re * v_im
                else:
                    t_re, t_im = m_re * v_re - m_im * v_im, m_re * v_im + m_im * v_re
                re, im = (t_re, t_im) if re is None else (re + t_re, im + t_im)
            k = 6 * chirality + a
            out_ref[k] = out_ref[k] + re if add else re
            out_ref[12 + k] = out_ref[12 + k] + im if add else im


def hop_terms(out_ref, links, ref, direction, weight_ahead, weight_behind, periodic):
    for row in range(2):
        ahead = half_spinor(ref, direction, row, -1)
        ahead = [tuple(shift(p, direction, 1, periodic) * weight_ahead for p in c) for c in ahead]
        forward = link_times(links, direction, ahead)
        behind = link_adjoint_times(links, direction, half_spinor(ref, direction, row, 1))
        behind = [tuple(shift(p, direction, -1, periodic) * weight_behind for p in c) for c in behind]
        add_hops(out_ref, direction, row, forward, behind)


def weights(direction, scale, outside=False):
    pair = []
    for offset in (1, -1):
        keep = inside(direction, offset)
        pair.append(jnp.where(keep, 0.0, scale) if outside else jnp.where(keep, scale, 0.0))
    return pair


def block_hops(out_ref, links, ref, weight_ref, x_periodic):
    for direction in range(4):
        if direction == 3 and x_periodic:
            hop_terms(out_ref, links, ref, 3, jnp.float32(-0.5), jnp.float32(-0.5), True)
        else:
            hop_terms(out_ref, links, ref, direction, weight_ref[2 * direction], weight_ref[2 * direction + 1], False)


def fill_weights(weight_ref):
    for direction in range(4):
        ahead, behind = weights(direction, -0.5)
        weight_ref[2 * direction] = ahead
        weight_ref[2 * direction + 1] = behind


def packed(vectors, direction, edge):
    flat = [part for vector in vectors for colour in vector for part in colour]
    tiles = []
    for group in range(3):
        tile = None
        for j in range(4):
            value = flat[4 * group + j]
            if direction == 0:
                moved, keep = roll(value, 4 * (j - edge), 0), iota(0) // 4 == j
            elif direction == 1:
                moved, keep = roll(value, j - edge, 0), iota(0) % 4 == j
            else:
                moved, keep = roll(value, LX * (j - edge), 1), iota(1) // LX == j
            tile = moved if tile is None else jnp.where(keep, moved, tile)
        tiles.append(tile)
    return tiles


def unpacked(tiles, direction, edge, scale):
    if direction == 0:
        weight = jnp.where(iota(0) // 4 == edge, scale, 0.0)
    elif direction == 1:
        weight = jnp.where(iota(0) % 4 == edge, scale, 0.0)
    else:
        weight = jnp.where(iota(1) // LX == edge, scale, 0.0)
    flat = []
    for group in range(3):
        for j in range(4):
            if direction == 0:
                moved = roll(tiles[group], 4 * (edge - j), 0)
            elif direction == 1:
                moved = roll(tiles[group], edge - j, 0)
            else:
                moved = roll(tiles[group], LX * (edge - j), 1)
            flat.append(moved * weight)
    pairs = [(flat[2 * k], flat[2 * k + 1]) for k in range(6)]
    return pairs[:3], pairs[3:]


def write_faces(face_refs, ref, links):
    for direction in range(3):
        up = packed(
            [link_adjoint_times(links, direction, half_spinor(ref, direction, row, 1)) for row in range(2)],
            direction, 3)
        down = packed([half_spinor(ref, direction, row, -1) for row in range(2)], direction, 0)
        even = lax.axis_index(AXES[direction]) % 2 == 0
        for group in range(3):
            rows = pl.ds(ROWS * group, ROWS)
            face_refs[MESSAGES.index((direction, 0))][rows] = jnp.where(even, up[group], down[group])
            face_refs[MESSAGES.index((direction, 1))][rows] = jnp.where(even, down[group], up[group])


def halo_hops(out_ref, links, face_refs):
    for direction in range(3):
        even = lax.axis_index(AXES[direction]) % 2 == 0
        above, below = [], []
        for group in range(3):
            rows = pl.ds(ROWS * group, ROWS)
            first, second = (face_refs[MESSAGES.index((direction, k))][rows] for k in range(2))
            above.append(jnp.where(even, first, second))
            below.append(jnp.where(even, second, first))
        scale_above = scale_below = jnp.float32(0.5)
        if direction == 0:
            place, last = lax.axis_index("ta"), lax.axis_size("ta") - 1
            scale_above = jnp.where(place == last, jnp.float32(-0.5), jnp.float32(0.5))
            scale_below = jnp.where(place == 0, jnp.float32(-0.5), jnp.float32(0.5))
        ahead = unpacked(above, direction, 3, scale_above)
        behind = unpacked(below, direction, 0, scale_below)
        for row in range(2):
            add_hops(out_ref, direction, row, link_times(links, direction, ahead[row]), behind[row])


def over_rows(value):
    for step in (4, 2, 1):
        value = value + roll(value, step, 0)
    return value


def turned(value, shift, stride):
    return pltpu.roll(value, shift, 1, stride=stride, stride_axis=0)


def block_total(value):
    total = over_rows(value[:8] + value[8:])
    row = lax.broadcasted_iota(jnp.int32, (8, LANES), 0)
    place = lax.broadcasted_iota(jnp.int32, (8, LANES), 1) % 4
    spread = None
    for shift, last in ((LX - 3, 7), (2 * LX - 3, 7), (3 * LX - 3, 7), (0, 7), (LANES - 7, 6)):
        source = place - (row + ((shift + 16) % LX - 16))
        part = jnp.where((source >= 0) & (source < 4) & (row <= last), turned(total, shift, 1), 0.0)
        spread = part if spread is None else spread + part
    return over_rows(spread)


def send_kernel(start_hbm, links_hbm, source_hbm, clover_hbm, start, links, source, clover, *rest):
    faces, sems = rest[:6], rest[6]
    near, far = pl.ds(0, 54), pl.ds(54, 18)
    copies = [
        pltpu.make_async_copy(start_hbm, start, sems.at[0]),
        pltpu.make_async_copy(links_hbm.at[near], links.at[near], sems.at[1]),
        pltpu.make_async_copy(links_hbm.at[far], links.at[far], sems.at[2]),
        pltpu.make_async_copy(source_hbm, source, sems.at[3]),
        pltpu.make_async_copy(clover_hbm, clover, sems.at[4]),
    ]
    for copy in copies:
        copy.start()
    copies[0].wait()
    copies[1].wait()
    write_faces(faces, start, links)
    for copy in copies[2:]:
        copy.wait()


def residual_kernel(source, start, links, clover, partial, source_sq, weight_ref):
    fill_weights(weight_ref)
    site_terms(partial, clover, start)
    block_hops(partial, links, start, weight_ref, True)
    total = None
    for k in range(24):
        value = source[k]
        partial[k] = value - partial[k]
        total = value * value if total is None else total + value * value
    source_sq[...] = total


def sweep_kernel(partial, links, clover, *rest):
    received, sent = rest[:6], rest[6:12]
    correction, remainder, applied, weight_ref = rest[12:]
    fill_weights(weight_ref)
    for k in range(24):
        remainder[k] = partial[k]
    halo_hops(remainder, links, received)

    for step in range(MR_STEPS):
        site_terms(applied, clover, remainder)
        block_hops(applied, links, remainder, weight_ref, False)
        dot_re = dot_im = norm = None
        for k in range(12):
            a_re, a_im, r_re, r_im = applied[k], applied[12 + k], remainder[k], remainder[12 + k]
            terms = (a_re * r_re + a_im * r_im, a_re * r_im - a_im * r_re, a_re * a_re + a_im * a_im)
            dot_re, dot_im, norm = terms if k == 0 else (dot_re + terms[0], dot_im + terms[1], norm + terms[2])
        norm = block_total(norm) + EPSILON
        alpha_re, alpha_im = block_total(dot_re) / norm, block_total(dot_im) / norm
        alpha_re = jnp.concatenate([alpha_re, alpha_re], axis=0)
        alpha_im = jnp.concatenate([alpha_im, alpha_im], axis=0)
        for k in range(12):
            a_re, a_im, r_re, r_im = applied[k], applied[12 + k], remainder[k], remainder[12 + k]
            gain_re, gain_im = alpha_re * r_re - alpha_im * r_im, alpha_re * r_im + alpha_im * r_re
            correction[k] = gain_re if step == 0 else correction[k] + gain_re
            correction[12 + k] = gain_im if step == 0 else correction[12 + k] + gain_im
            remainder[k] = r_re - (alpha_re * a_re - alpha_im * a_im)
            remainder[12 + k] = r_im - (alpha_re * a_im + alpha_im * a_re)
    write_faces(sent, correction, links)


def inner_kernel(start, correction, remainder, links, update_hbm, latest, update, sem):
    for k in range(24):
        update[k] = start[k] + correction[k]
        latest[k] = remainder[k]
    copy = pltpu.make_async_copy(update, update_hbm, sem)
    copy.start()
    ahead, behind = weights(3, 0.5, outside=True)
    hop_terms(latest, links, correction, 3, ahead, behind, True)
    copy.wait()


def latest_kernel(partial, source_sq, links, *rest):
    received, sums, latest = rest[:6], rest[6], rest[7]
    for k in range(24):
        latest[k] = partial[k]
    halo_hops(latest, links, received)
    total = None
    for k in range(24):
        square = latest[k] * latest[k]
        total = square if total is None else total + square
    row = lax.broadcasted_iota(jnp.int32, (8, LANES), 0)
    lane = lax.broadcasted_iota(jnp.int32, (8, LANES), 1)
    summed = None
    for j, value in enumerate((total, source_sq[...])):
        for t in range(4):
            half = value[8 * (t // 2):8 * (t // 2) + 8]
            part = turned(over_rows(jnp.where(row // 4 == t % 2, half, 0.0)), 0, 1)
            summed = part if summed is None else jnp.where(lane % 8 == 4 * j + t, part, summed)
    summed = over_rows(summed)[:1]
    for k in range(sums.shape[0]):
        sums[k] = summed


def profile_kernel(gathered, profile):
    total = gathered[0]
    for k in range(1, gathered.shape[0]):
        total = total + gathered[k]
    total = jnp.broadcast_to(total, (8, LANES))
    residual = over_rows(turned(total, 0, 8) + turned(total, 64, 8))
    source = over_rows(turned(total, 4, 8) + turned(total, 68, 8))
    profile[...] = (residual / source)[:1, :4]


PARAMS = pltpu.CompilerParams(vmem_limit_bytes=12 * 2**20)
FIELD = pltpu.VMEM((24, ROWS, LANES), jnp.float32)
FACE = pltpu.VMEM((48, LANES), jnp.float32)
SCRATCH = pltpu.VMEM((24, ROWS, LANES), jnp.float32)
IN_HBM = pl.BlockSpec(memory_space=pltpu.HBM)
WEIGHTS = pltpu.VMEM((8, ROWS, LANES), jnp.float32)


def in_vmem(value):
    return pltpu.with_memory_space_constraint(value, pltpu.VMEM)


def in_hbm(value):
    return pltpu.with_memory_space_constraint(value, pltpu.HBM)


def call(body, outs, scratch=(), flops=10_000_000):
    kernel = pl.pallas_call(
        body,
        out_shape=outs,
        scratch_shapes=scratch,
        compiler_params=PARAMS,
        cost_estimate=pl.CostEstimate(flops=flops, transcendentals=0, bytes_accessed=2_000_000),
    )
    return lambda *args: kernel(*map(in_vmem, args))


def matching(count, first):
    pairs = []
    for low in range(first, count + first, 2):
        a, b = low % count, (low + 1) % count
        pairs += [(a, b), (b, a)]
    return pairs


def exchange(faces):
    received = []
    for face, (direction, first) in zip(faces, MESSAGES):
        axis = AXES[direction]
        received.append(lax.ppermute(face, axis, matching(lax.axis_size(axis), first)))
    return received


def local(source, start_guess, gauge_links, clover):
    shape = source.shape
    source = source.reshape(24, ROWS, LANES)
    start = start_guess.reshape(24, ROWS, LANES)
    links = gauge_links.reshape(72, ROWS, LANES)
    clover = clover.reshape(144, ROWS, LANES)
    start, links, source, clover, *faces = pl.pallas_call(
        send_kernel,
        in_specs=[IN_HBM] * 4,
        out_shape=[FIELD, pltpu.VMEM(links.shape, jnp.float32), FIELD, pltpu.VMEM(clover.shape, jnp.float32)]
        + [FACE] * 6,
        scratch_shapes=[pltpu.SemaphoreType.DMA((5,))],
        compiler_params=PARAMS,
    )(in_hbm(start), in_hbm(links), in_hbm(source), in_hbm(clover))
    received = exchange(faces)
    partial, source_sq = call(residual_kernel, [FIELD, pltpu.VMEM((ROWS, LANES), jnp.float32)], [WEIGHTS])(
        source, start, links, clover)
    *faces, correction, remainder = call(sweep_kernel, [FACE] * 6 + [FIELD] * 2, [SCRATCH, WEIGHTS])(
        partial, links, clover, *received)
    received = exchange(faces)
    update, latest = call(
        inner_kernel, [pltpu.HBM(source.shape, jnp.float32), FIELD], [SCRATCH, pltpu.SemaphoreType.DMA(())])(
            start, correction, remainder, links)
    group = GZ + ("gy",)
    sums = call(latest_kernel, pltpu.VMEM((lax.axis_size(group), 1, LANES), jnp.float32), [SCRATCH])(
        latest, source_sq, links, *received)
    sums = lax.all_to_all(sums, group, 0, 0)
    profile = call(profile_kernel, jax.ShapeDtypeStruct((1, 4), jnp.float32))(sums)
    return update.reshape(shape), profile.reshape(4)


def solution(mesh):
    finer = Mesh(
        mesh.devices.reshape(mesh.shape["ta"], 2, 2, mesh.shape["gy"]), ("ta", "gz_0", "gz_1", "gy")
    )
    field = P(None, None, None, "ta", GZ, "gy")
    matrix = P(None, None, None, None, "ta", GZ, "gy")
    return jax.shard_map(
        local, mesh=finer, in_specs=(field, field, matrix, matrix), out_specs=(field, P("ta")), check_vma=False
    )
```

```python
import jax
import jax.numpy as jnp
from jax import lax
from jax.experimental import pallas as pl
from jax.experimental.pallas import tpu as pltpu
from jax.sharding import Mesh
from jax.sharding import PartitionSpec as P

LX = 32
MR_STEPS = 4
EPSILON = 1e-06
GZ = ("gz_0", "gz_1")
ROWS, LANES = 16, 128
AXES = ("ta", GZ, "gy")
MESSAGES = ((0, 1), (0, 0), (2, 1), (2, 0), (1, 1), (1, 0))

UPPER = (
    ((0, 1), (1, 1)),
    ((0, -1j), (1, 1j)),
    ((1, -1), (0, 1)),
    ((1, -1j), (0, -1j)),
)


def plus(a, b):
    return a[0] + b[0], a[1] + b[1]


def plus_times(a, coef, b):
    if coef == 1:
        return a[0] + b[0], a[1] + b[1]
    if coef == -1:
        return a[0] - b[0], a[1] - b[1]
    if coef == 1j:
        return a[0] - b[1], a[1] + b[0]
    return a[0] + b[1], a[1] - b[0]


def iota(axis):
    return lax.broadcasted_iota(jnp.int32, (ROWS, LANES), axis)


def roll(value, shift, axis):
    size = value.shape[axis]
    shift = shift % size
    if shift == 0:
        return value
    return pltpu.roll(value, shift, axis)


def spinor_at(ref, spin, colour, rows=slice(None)):
    return ref[3 * spin + colour, rows], ref[12 + 3 * spin + colour, rows]


def half_spinor(ref, direction, row, sign, rows=slice(None)):
    column, entry = UPPER[direction][row]
    return [
        plus_times(spinor_at(ref, row, colour, rows), sign * entry, spinor_at(ref, 2 + column, colour, rows))
        for colour in range(3)
    ]


def link_at(links, direction, row, column, rows=slice(None)):
    base = 18 * direction + 3 * row + column
    return links[base, rows], links[base + 9, rows]


def link_times(links, direction, vector, rows=slice(None)):
    out = []
    for row in range(3):
        re = im = None
        for column in range(3):
            u_re, u_im = link_at(links, direction, row, column, rows)
            v_re, v_im = vector[column]
            t_re, t_im = u_re * v_re - u_im * v_im, u_re * v_im + u_im * v_re
            re, im = (t_re, t_im) if re is None else (re + t_re, im + t_im)
        out.append((re, im))
    return out


def link_adjoint_times(links, direction, vector, rows=slice(None)):
    out = []
    for row in range(3):
        re = im = None
        for column in range(3):
            u_re, u_im = link_at(links, direction, column, row, rows)
            v_re, v_im = vector[column]
            t_re, t_im = u_re * v_re + u_im * v_im, u_re * v_im - u_im * v_re
            re, im = (t_re, t_im) if re is None else (re + t_re, im + t_im)
        out.append((re, im))
    return out


def add_hops(out_ref, direction, row, forward, behind):
    column, entry = UPPER[direction][row]
    conj = complex(entry).conjugate()
    for colour in range(3):
        upper = plus(forward[colour], behind[colour])
        lower = plus_times(behind[colour], -1, forward[colour])
        for spin, coef, value in ((row, 1, upper), (2 + column, conj, lower)):
            k = 3 * spin + colour
            out_ref[k], out_ref[12 + k] = plus_times((out_ref[k], out_ref[12 + k]), coef, value)


def shift(value, direction, offset, periodic):
    if direction == 0:
        low, high = roll(value[:8], 4, 0), roll(value[8:], 4, 0)
        front = lax.broadcasted_iota(jnp.int32, (8, LANES), 0) < 4
        if offset > 0:
            return jnp.concatenate([jnp.where(front, low, high), high], axis=0)
        return jnp.concatenate([jnp.where(front, high, low), jnp.where(front, low, high)], axis=0)
    if direction == 1:
        return jnp.concatenate([roll(value[:8], -offset, 0), roll(value[8:], -offset, 0)], axis=0)
    if direction == 2:
        return roll(value, -LX * offset, 1)
    near = roll(value, -offset, 1)
    if not periodic:
        return near
    edge = (LX - 1) if offset > 0 else 0
    return jnp.where(iota(1) % LX == edge, roll(value, offset * (LX - 1), 1), near)


def inside(direction, offset):
    edge = 3 if offset > 0 else 0
    if direction == 0:
        return iota(0) // 4 != edge
    if direction == 1:
        return iota(0) % 4 != edge
    if direction == 2:
        return iota(1) // LX != edge
    return iota(1) % 4 != edge


def site_terms(out_ref, clover, ref, add=False):
    for chirality in range(2):
        for a in range(6):
            re = im = None
            for b in range(6):
                base = 72 * chirality + 6 * a + b
                m_re, m_im = clover[base], clover[base + 36]
                v_re, v_im = ref[6 * chirality + b], ref[12 + 6 * chirality + b]
                if a == b:
                    t_re, t_im = m_re * v_re, m_re * v_im
                else:
                    t_re, t_im = m_re * v_re - m_im * v_im, m_re * v_im + m_im * v_re
                re, im = (t_re, t_im) if re is None else (re + t_re, im + t_im)
            k = 6 * chirality + a
            out_ref[k] = out_ref[k] + re if add else re
            out_ref[12 + k] = out_ref[12 + k] + im if add else im


def hop_terms(out_ref, links, ref, direction, ahead_weight=None, behind_weight=None, periodic=False):
    for row in range(2):
        ahead = half_spinor(ref, direction, row, -1)
        ahead = [tuple(shift(p, direction, 1, periodic) for p in c) for c in ahead]
        forward = link_times(links, direction, ahead)
        behind = link_adjoint_times(links, direction, half_spinor(ref, direction, row, 1))
        behind = [tuple(shift(p, direction, -1, periodic) for p in c) for c in behind]
        if ahead_weight is not None:
            forward = [tuple(p * ahead_weight for p in c) for c in forward]
            behind = [tuple(p * behind_weight for p in c) for c in behind]
        add_hops(out_ref, direction, row, forward, behind)


def outside(direction, scale):
    return [jnp.where(inside(direction, offset), jnp.float32(0.0), jnp.float32(scale)) for offset in (1, -1)]


def cut_links(block_links, links):
    for direction in range(4):
        weight = jnp.where(inside(direction, 1), jnp.float32(-0.5), jnp.float32(0.0))
        for k in range(18):
            block_links[18 * direction + k] = links[18 * direction + k] * weight


def block_operator(out_ref, clover, block_links, ref):
    site_terms(out_ref, clover, ref)
    for direction in range(4):
        hop_terms(out_ref, block_links, ref, direction)


def packed(vectors, direction, edge):
    flat = [part for vector in vectors for colour in vector for part in colour]
    tiles = []
    for group in range(3):
        tile = None
        for j in range(4):
            value = flat[4 * group + j]
            if direction == 0:
                moved, keep = roll(value, 4 * (j - edge), 0), iota(0) // 4 == j
            elif direction == 1:
                moved, keep = roll(value, j - edge, 0), iota(0) % 4 == j
            else:
                moved, keep = roll(value, LX * (j - edge), 1), iota(1) // LX == j
            tile = moved if tile is None else jnp.where(keep, moved, tile)
        tiles.append(tile)
    return tiles


def unpacked(tiles, direction, edge, scale):
    if direction == 0:
        weight = jnp.where(iota(0) // 4 == edge, scale, 0.0)
    elif direction == 1:
        weight = jnp.where(iota(0) % 4 == edge, scale, 0.0)
    else:
        weight = jnp.where(iota(1) // LX == edge, scale, 0.0)
    flat = []
    for group in range(3):
        for j in range(4):
            if direction == 0:
                moved = roll(tiles[group], 4 * (edge - j), 0)
            elif direction == 1:
                moved = roll(tiles[group], edge - j, 0)
            else:
                moved = roll(tiles[group], LX * (edge - j), 1)
            flat.append(moved * weight)
    pairs = [(flat[2 * k], flat[2 * k + 1]) for k in range(6)]
    return pairs[:3], pairs[3:]


def write_faces(face_refs, ref, links):
    for direction in range(3):
        up = packed(
            [link_adjoint_times(links, direction, half_spinor(ref, direction, row, 1)) for row in range(2)],
            direction, 3)
        down = packed([half_spinor(ref, direction, row, -1) for row in range(2)], direction, 0)
        even = lax.axis_index(AXES[direction]) % 2 == 0
        for group in range(3):
            rows = pl.ds(ROWS * group, ROWS)
            face_refs[MESSAGES.index((direction, 0))][rows] = jnp.where(even, up[group], down[group])
            face_refs[MESSAGES.index((direction, 1))][rows] = jnp.where(even, down[group], up[group])


def halo_hops(out_ref, links, face_refs):
    for direction in range(3):
        even = lax.axis_index(AXES[direction]) % 2 == 0
        above, below = [], []
        for group in range(3):
            rows = pl.ds(ROWS * group, ROWS)
            first, second = (face_refs[MESSAGES.index((direction, k))][rows] for k in range(2))
            above.append(jnp.where(even, first, second))
            below.append(jnp.where(even, second, first))
        scale_above = scale_below = jnp.float32(0.5)
        if direction == 0:
            place, last = lax.axis_index("ta"), lax.axis_size("ta") - 1
            scale_above = jnp.where(place == last, jnp.float32(-0.5), jnp.float32(0.5))
            scale_below = jnp.where(place == 0, jnp.float32(-0.5), jnp.float32(0.5))
        ahead = unpacked(above, direction, 3, scale_above)
        behind = unpacked(below, direction, 0, scale_below)
        for row in range(2):
            add_hops(out_ref, direction, row, link_times(links, direction, ahead[row]), behind[row])


def over_rows(value):
    for step in (4, 2, 1):
        value = value + roll(value, step, 0)
    return value


def turned(value, shift, stride):
    return pltpu.roll(value, shift, 1, stride=stride, stride_axis=0)


def block_total(value):
    total = over_rows(value[:8] + value[8:])
    row = lax.broadcasted_iota(jnp.int32, (8, LANES), 0)
    place = lax.broadcasted_iota(jnp.int32, (8, LANES), 1) % 4
    spread = None
    for shift, last in ((LX - 3, 7), (2 * LX - 3, 7), (3 * LX - 3, 7), (0, 7), (LANES - 7, 6)):
        source = place - (row + ((shift + 16) % LX - 16))
        part = jnp.where((source >= 0) & (source < 4) & (row <= last), turned(total, shift, 1), 0.0)
        spread = part if spread is None else spread + part
    return over_rows(spread)


def send_kernel(start_hbm, links_hbm, source_hbm, clover_hbm, start, links, source, clover, *rest):
    faces, sems = rest[:6], rest[6]
    near, far = pl.ds(0, 54), pl.ds(54, 18)
    copies = [
        pltpu.make_async_copy(start_hbm, start, sems.at[0]),
        pltpu.make_async_copy(links_hbm.at[near], links.at[near], sems.at[1]),
        pltpu.make_async_copy(links_hbm.at[far], links.at[far], sems.at[2]),
        pltpu.make_async_copy(source_hbm, source, sems.at[3]),
        pltpu.make_async_copy(clover_hbm, clover, sems.at[4]),
    ]
    for copy in copies:
        copy.start()
    copies[0].wait()
    copies[1].wait()
    write_faces(faces, start, links)
    for copy in copies[2:]:
        copy.wait()


def residual_kernel(source, start, links, clover, partial, source_sq, block_links):
    cut_links(block_links, links)
    site_terms(partial, clover, start)
    for direction in range(3):
        hop_terms(partial, block_links, start, direction)
    half = jnp.float32(-0.5)
    hop_terms(partial, links, start, 3, half, half, True)
    total = None
    for k in range(24):
        value = source[k]
        partial[k] = value - partial[k]
        total = value * value if total is None else total + value * value
    source_sq[...] = total


def sweep_kernel(partial, start, links, block_links, clover, *rest):
    received, sent = rest[:6], rest[6:12]
    correction, remainder, update, applied, again = rest[12:]
    for k in range(24):
        remainder[k] = partial[k]
    halo_hops(remainder, links, received)
    block_operator(applied, clover, block_links, remainder)
    for step in range(MR_STEPS):
        dot_re = dot_im = norm = None
        for k in range(12):
            a_re, a_im, r_re, r_im = applied[k], applied[12 + k], remainder[k], remainder[12 + k]
            terms = (a_re * r_re + a_im * r_im, a_re * r_im - a_im * r_re, a_re * a_re + a_im * a_im)
            dot_re, dot_im, norm = terms if k == 0 else (dot_re + terms[0], dot_im + terms[1], norm + terms[2])
        norm = block_total(norm) + EPSILON
        alpha_re, alpha_im = block_total(dot_re) / norm, block_total(dot_im) / norm
        alpha_re = jnp.concatenate([alpha_re, alpha_re], axis=0)
        alpha_im = jnp.concatenate([alpha_im, alpha_im], axis=0)
        last = step == MR_STEPS - 1
        if not last:
            block_operator(again, clover, block_links, applied)
        for k in range(12):
            a_re, a_im, r_re, r_im = applied[k], applied[12 + k], remainder[k], remainder[12 + k]
            gain_re, gain_im = alpha_re * r_re - alpha_im * r_im, alpha_re * r_im + alpha_im * r_re
            correction[k] = gain_re if step == 0 else correction[k] + gain_re
            correction[12 + k] = gain_im if step == 0 else correction[12 + k] + gain_im
            remainder[k] = r_re - (alpha_re * a_re - alpha_im * a_im)
            remainder[12 + k] = r_im - (alpha_re * a_im + alpha_im * a_re)
            if not last:
                b_re, b_im = again[k], again[12 + k]
                applied[k] = a_re - (alpha_re * b_re - alpha_im * b_im)
                applied[12 + k] = a_im - (alpha_re * b_im + alpha_im * b_re)
    write_faces(sent, correction, links)
    for k in range(24):
        update[k] = start[k] + correction[k]


def inner_kernel(update, correction, remainder, links, update_hbm, latest, sem):
    copy = pltpu.make_async_copy(update, update_hbm, sem)
    copy.start()
    for k in range(24):
        latest[k] = remainder[k]
    ahead, behind = outside(3, 0.5)
    hop_terms(latest, links, correction, 3, ahead, behind, True)
    copy.wait()


def latest_kernel(partial, source_sq, links, *rest):
    received, sums, latest = rest[:6], rest[6], rest[7]
    for k in range(24):
        latest[k] = partial[k]
    halo_hops(latest, links, received)
    total = None
    for k in range(24):
        square = latest[k] * latest[k]
        total = square if total is None else total + square
    row = lax.broadcasted_iota(jnp.int32, (8, LANES), 0)
    lane = lax.broadcasted_iota(jnp.int32, (8, LANES), 1)
    summed = None
    for j, value in enumerate((total, source_sq[...])):
        for t in range(4):
            half = value[8 * (t // 2):8 * (t // 2) + 8]
            part = turned(over_rows(jnp.where(row // 4 == t % 2, half, 0.0)), 0, 1)
            summed = part if summed is None else jnp.where(lane % 8 == 4 * j + t, part, summed)
    summed = over_rows(summed)[:1]
    for k in range(sums.shape[0]):
        sums[k] = summed


def profile_kernel(gathered, profile):
    total = gathered[0]
    for k in range(1, gathered.shape[0]):
        total = total + gathered[k]
    total = jnp.broadcast_to(total, (8, LANES))
    residual = over_rows(turned(total, 0, 8) + turned(total, 64, 8))
    source = over_rows(turned(total, 4, 8) + turned(total, 68, 8))
    profile[...] = (residual / source)[:1, :4]


PARAMS = pltpu.CompilerParams(vmem_limit_bytes=12 * 2**20)
FIELD = pltpu.VMEM((24, ROWS, LANES), jnp.float32)
FACE = pltpu.VMEM((48, LANES), jnp.float32)
SCRATCH = pltpu.VMEM((24, ROWS, LANES), jnp.float32)
IN_HBM = pl.BlockSpec(memory_space=pltpu.HBM)
LINKS = pltpu.VMEM((72, ROWS, LANES), jnp.float32)


def in_vmem(value):
    return pltpu.with_memory_space_constraint(value, pltpu.VMEM)


def in_hbm(value):
    return pltpu.with_memory_space_constraint(value, pltpu.HBM)


def call(body, outs, scratch=(), flops=10_000_000):
    kernel = pl.pallas_call(
        body,
        out_shape=outs,
        scratch_shapes=scratch,
        compiler_params=PARAMS,
        cost_estimate=pl.CostEstimate(flops=flops, transcendentals=0, bytes_accessed=2_000_000),
    )
    return lambda *args: kernel(*map(in_vmem, args))


def matching(count, first):
    pairs = []
    for low in range(first, count + first, 2):
        a, b = low % count, (low + 1) % count
        pairs += [(a, b), (b, a)]
    return pairs


def exchange(faces):
    received = []
    for face, (direction, first) in zip(faces, MESSAGES):
        axis = AXES[direction]
        received.append(lax.ppermute(face, axis, matching(lax.axis_size(axis), first)))
    return received


def local(source, start_guess, gauge_links, clover):
    shape = source.shape
    source = source.reshape(24, ROWS, LANES)
    start = start_guess.reshape(24, ROWS, LANES)
    links = gauge_links.reshape(72, ROWS, LANES)
    clover = clover.reshape(144, ROWS, LANES)
    start, links, source, clover, *faces = pl.pallas_call(
        send_kernel,
        in_specs=[IN_HBM] * 4,
        out_shape=[FIELD, LINKS, FIELD, pltpu.VMEM(clover.shape, jnp.float32)]
        + [FACE] * 6,
        scratch_shapes=[pltpu.SemaphoreType.DMA((5,))],
        compiler_params=PARAMS,
    )(in_hbm(start), in_hbm(links), in_hbm(source), in_hbm(clover))
    received = exchange(faces)
    partial, source_sq, block_links = call(
        residual_kernel, [FIELD, pltpu.VMEM((ROWS, LANES), jnp.float32), LINKS])(source, start, links, clover)
    *faces, correction, remainder, update = call(sweep_kernel, [FACE] * 6 + [FIELD] * 3, [SCRATCH] * 2)(
        partial, start, links, block_links, clover, *received)
    received = exchange(faces)
    update, latest = call(
        inner_kernel, [pltpu.HBM(source.shape, jnp.float32), FIELD], [pltpu.SemaphoreType.DMA(())])(
            update, correction, remainder, links)
    group = GZ + ("gy",)
    sums = call(latest_kernel, pltpu.VMEM((lax.axis_size(group), 1, LANES), jnp.float32), [SCRATCH])(
        latest, source_sq, links, *received)
    sums = lax.all_to_all(sums, group, 0, 0)
    profile = call(profile_kernel, jax.ShapeDtypeStruct((1, 4), jnp.float32))(sums)
    return update.reshape(shape), profile.reshape(4)


def solution(mesh):
    finer = Mesh(
        mesh.devices.reshape(mesh.shape["ta"], 2, 2, mesh.shape["gy"]), ("ta", "gz_0", "gz_1", "gy")
    )
    field = P(None, None, None, "ta", GZ, "gy")
    matrix = P(None, None, None, None, "ta", GZ, "gy")
    return jax.shard_map(
        local, mesh=finer, in_specs=(field, field, matrix, matrix), out_specs=(field, P("ta")), check_vma=False
    )
```

```python
import jax
import jax.numpy as jnp
from jax import lax
from jax.experimental import pallas as pl
from jax.experimental.pallas import tpu as pltpu
from jax.sharding import Mesh
from jax.sharding import PartitionSpec as P

LX = 32
MR_STEPS = 4
EPSILON = 1e-06
GZ = ("gz_0", "gz_1")
ROWS, LANES = 16, 128
AXES = ("ta", GZ, "gy")
MESSAGES = ((0, 1), (0, 0), (2, 1), (2, 0), (1, 1), (1, 0))

UPPER = (
    ((0, 1), (1, 1)),
    ((0, -1j), (1, 1j)),
    ((1, -1), (0, 1)),
    ((1, -1j), (0, -1j)),
)


def plus(a, b):
    return a[0] + b[0], a[1] + b[1]


def plus_times(a, coef, b):
    if coef == 1:
        return a[0] + b[0], a[1] + b[1]
    if coef == -1:
        return a[0] - b[0], a[1] - b[1]
    if coef == 1j:
        return a[0] - b[1], a[1] + b[0]
    return a[0] + b[1], a[1] - b[0]


def iota(axis):
    return lax.broadcasted_iota(jnp.int32, (ROWS, LANES), axis)


def roll(value, shift, axis):
    size = value.shape[axis]
    shift = shift % size
    if shift == 0:
        return value
    return pltpu.roll(value, shift, axis)


def spinor_at(ref, spin, colour, rows=slice(None)):
    return ref[3 * spin + colour, rows], ref[12 + 3 * spin + colour, rows]


def half_spinor(ref, direction, row, sign, rows=slice(None)):
    column, entry = UPPER[direction][row]
    return [
        plus_times(spinor_at(ref, row, colour, rows), sign * entry, spinor_at(ref, 2 + column, colour, rows))
        for colour in range(3)
    ]


def link_at(links, direction, row, column, rows=slice(None)):
    base = 18 * direction + 3 * row + column
    return links[base, rows], links[base + 9, rows]


def link_times(links, direction, vector, rows=slice(None)):
    out = []
    for row in range(3):
        re = im = None
        for column in range(3):
            u_re, u_im = link_at(links, direction, row, column, rows)
            v_re, v_im = vector[column]
            t_re, t_im = u_re * v_re - u_im * v_im, u_re * v_im + u_im * v_re
            re, im = (t_re, t_im) if re is None else (re + t_re, im + t_im)
        out.append((re, im))
    return out


def link_adjoint_times(links, direction, vector, rows=slice(None)):
    out = []
    for row in range(3):
        re = im = None
        for column in range(3):
            u_re, u_im = link_at(links, direction, column, row, rows)
            v_re, v_im = vector[column]
            t_re, t_im = u_re * v_re + u_im * v_im, u_re * v_im - u_im * v_re
            re, im = (t_re, t_im) if re is None else (re + t_re, im + t_im)
        out.append((re, im))
    return out


def add_hops(out_ref, direction, row, forward, behind):
    column, entry = UPPER[direction][row]
    conj = complex(entry).conjugate()
    for colour in range(3):
        upper = plus(forward[colour], behind[colour])
        lower = plus_times(behind[colour], -1, forward[colour])
        for spin, coef, value in ((row, 1, upper), (2 + column, conj, lower)):
            k = 3 * spin + colour
            out_ref[k], out_ref[12 + k] = plus_times((out_ref[k], out_ref[12 + k]), coef, value)


def shift(value, direction, offset, periodic):
    if direction == 0:
        low, high = roll(value[:8], 4, 0), roll(value[8:], 4, 0)
        front = lax.broadcasted_iota(jnp.int32, (8, LANES), 0) < 4
        if offset > 0:
            return jnp.concatenate([jnp.where(front, low, high), high], axis=0)
        return jnp.concatenate([jnp.where(front, high, low), jnp.where(front, low, high)], axis=0)
    if direction == 1:
        return jnp.concatenate([roll(value[:8], -offset, 0), roll(value[8:], -offset, 0)], axis=0)
    if direction == 2:
        return roll(value, -LX * offset, 1)
    near = roll(value, -offset, 1)
    if not periodic:
        return near
    edge = (LX - 1) if offset > 0 else 0
    return jnp.where(iota(1) % LX == edge, roll(value, offset * (LX - 1), 1), near)


def inside(direction, offset):
    edge = 3 if offset > 0 else 0
    if direction == 0:
        return iota(0) // 4 != edge
    if direction == 1:
        return iota(0) % 4 != edge
    if direction == 2:
        return iota(1) // LX != edge
    return iota(1) % 4 != edge


def clover_runs():
    runs, kept = [], 0
    for chirality in range(2):
        for part in range(2):
            for a in range(6 - part):
                runs.append((72 * chirality + 36 * part + 7 * a + part, kept, 6 - part - a))
                kept += 6 - part - a
    return runs


KEPT = {first + k: kept + k for first, kept, rows in clover_runs() for k in range(rows)}


def site_terms(out_ref, clover, ref):
    for chirality in range(2):
        for a in range(6):
            re = im = None
            for b in range(6):
                place = 72 * chirality + 6 * min(a, b) + max(a, b)
                m_re = clover[KEPT[place]]
                v_re, v_im = ref[6 * chirality + b], ref[12 + 6 * chirality + b]
                t_re, t_im = m_re * v_re, m_re * v_im
                re, im = (t_re, t_im) if re is None else (re + t_re, im + t_im)
                if a != b:
                    m_im = clover[KEPT[place + 36]]
                    if a < b:
                        re, im = re - m_im * v_im, im + m_im * v_re
                    else:
                        re, im = re + m_im * v_im, im - m_im * v_re
            k = 6 * chirality + a
            out_ref[k] = re
            out_ref[12 + k] = im


def hop_terms(out_ref, links, ref, direction, ahead_weight=None, behind_weight=None, periodic=False):
    for row in range(2):
        ahead = half_spinor(ref, direction, row, -1)
        ahead = [tuple(shift(p, direction, 1, periodic) for p in c) for c in ahead]
        forward = link_times(links, direction, ahead)
        behind = link_adjoint_times(links, direction, half_spinor(ref, direction, row, 1))
        behind = [tuple(shift(p, direction, -1, periodic) for p in c) for c in behind]
        if ahead_weight is not None:
            forward = [tuple(p * ahead_weight for p in c) for c in forward]
            behind = [tuple(p * behind_weight for p in c) for c in behind]
        add_hops(out_ref, direction, row, forward, behind)


def outside(direction, scale):
    return [jnp.where(inside(direction, offset), jnp.float32(0.0), jnp.float32(scale)) for offset in (1, -1)]


def cut_links(block_links, links):
    for direction in range(4):
        weight = jnp.where(inside(direction, 1), jnp.float32(-0.5), jnp.float32(0.0))
        for k in range(18):
            block_links[18 * direction + k] = links[18 * direction + k] * weight


def block_operator(out_ref, clover, block_links, ref):
    site_terms(out_ref, clover, ref)
    for direction in range(4):
        hop_terms(out_ref, block_links, ref, direction)


def packed(vectors, direction, edge):
    flat = [part for vector in vectors for colour in vector for part in colour]
    tiles = []
    for group in range(3):
        tile = None
        for j in range(4):
            value = flat[4 * group + j]
            if direction == 0:
                moved, keep = roll(value, 4 * (j - edge), 0), iota(0) // 4 == j
            elif direction == 1:
                moved, keep = roll(value, j - edge, 0), iota(0) % 4 == j
            else:
                moved, keep = roll(value, LX * (j - edge), 1), iota(1) // LX == j
            tile = moved if tile is None else jnp.where(keep, moved, tile)
        tiles.append(tile)
    return tiles


def unpacked(tiles, direction, edge, scale):
    if direction == 0:
        weight = jnp.where(iota(0) // 4 == edge, scale, 0.0)
    elif direction == 1:
        weight = jnp.where(iota(0) % 4 == edge, scale, 0.0)
    else:
        weight = jnp.where(iota(1) // LX == edge, scale, 0.0)
    flat = []
    for group in range(3):
        for j in range(4):
            if direction == 0:
                moved = roll(tiles[group], 4 * (edge - j), 0)
            elif direction == 1:
                moved = roll(tiles[group], edge - j, 0)
            else:
                moved = roll(tiles[group], LX * (edge - j), 1)
            flat.append(moved * weight)
    pairs = [(flat[2 * k], flat[2 * k + 1]) for k in range(6)]
    return pairs[:3], pairs[3:]


def write_faces(face_refs, ref, links):
    for direction in range(3):
        up = packed(
            [link_adjoint_times(links, direction, half_spinor(ref, direction, row, 1)) for row in range(2)],
            direction, 3)
        down = packed([half_spinor(ref, direction, row, -1) for row in range(2)], direction, 0)
        even = lax.axis_index(AXES[direction]) % 2 == 0
        for group in range(3):
            rows = pl.ds(ROWS * group, ROWS)
            face_refs[MESSAGES.index((direction, 0))][rows] = jnp.where(even, up[group], down[group])
            face_refs[MESSAGES.index((direction, 1))][rows] = jnp.where(even, down[group], up[group])


def halo_hops(out_ref, links, face_refs):
    for direction in range(3):
        even = lax.axis_index(AXES[direction]) % 2 == 0
        above, below = [], []
        for group in range(3):
            rows = pl.ds(ROWS * group, ROWS)
            first, second = (face_refs[MESSAGES.index((direction, k))][rows] for k in range(2))
            above.append(jnp.where(even, first, second))
            below.append(jnp.where(even, second, first))
        scale_above = scale_below = jnp.float32(0.5)
        if direction == 0:
            place, last = lax.axis_index("ta"), lax.axis_size("ta") - 1
            scale_above = jnp.where(place == last, jnp.float32(-0.5), jnp.float32(0.5))
            scale_below = jnp.where(place == 0, jnp.float32(-0.5), jnp.float32(0.5))
        ahead = unpacked(above, direction, 3, scale_above)
        behind = unpacked(below, direction, 0, scale_below)
        for row in range(2):
            add_hops(out_ref, direction, row, link_times(links, direction, ahead[row]), behind[row])


def over_rows(value):
    for step in (4, 2, 1):
        value = value + roll(value, step, 0)
    return value


def turned(value, shift, stride):
    return pltpu.roll(value, shift, 1, stride=stride, stride_axis=0)


def block_total(value):
    total = over_rows(value[:8] + value[8:])
    row = lax.broadcasted_iota(jnp.int32, (8, LANES), 0)
    place = lax.broadcasted_iota(jnp.int32, (8, LANES), 1) % 4
    spread = None
    for shift, last in ((LX - 3, 7), (2 * LX - 3, 7), (3 * LX - 3, 7), (0, 7), (LANES - 7, 6)):
        source = place - (row + ((shift + 16) % LX - 16))
        part = jnp.where((source >= 0) & (source < 4) & (row <= last), turned(total, shift, 1), 0.0)
        spread = part if spread is None else spread + part
    return over_rows(spread)


def send_kernel(start_hbm, links_hbm, source_hbm, clover_hbm, start, links, source, clover, *rest):
    faces, sems = rest[:6], rest[6]
    near, far = pl.ds(0, 54), pl.ds(54, 18)
    copies = [
        pltpu.make_async_copy(start_hbm, start, sems.at[0]),
        pltpu.make_async_copy(links_hbm.at[near], links.at[near], sems.at[1]),
        pltpu.make_async_copy(links_hbm.at[far], links.at[far], sems.at[2]),
        pltpu.make_async_copy(source_hbm, source, sems.at[3]),
    ]
    for k, (first, kept, rows) in enumerate(clover_runs()):
        copies.append(
            pltpu.make_async_copy(clover_hbm.at[pl.ds(first, rows)], clover.at[pl.ds(kept, rows)], sems.at[4 + k]))
    for copy in copies:
        copy.start()
    copies[0].wait()
    copies[1].wait()
    write_faces(faces, start, links)
    for copy in copies[2:]:
        copy.wait()


def residual_kernel(source, start, links, clover, partial, source_sq, block_links):
    cut_links(block_links, links)
    site_terms(partial, clover, start)
    for direction in range(3):
        hop_terms(partial, block_links, start, direction)
    half = jnp.float32(-0.5)
    hop_terms(partial, links, start, 3, half, half, True)
    total = None
    for k in range(24):
        value = source[k]
        partial[k] = value - partial[k]
        total = value * value if total is None else total + value * value
    source_sq[...] = total


def sweep_kernel(partial, start, links, block_links, clover, *rest):
    received, sent = rest[:6], rest[6:12]
    correction, remainder, update, applied, again = rest[12:]
    for k in range(24):
        remainder[k] = partial[k]
    halo_hops(remainder, links, received)
    block_operator(applied, clover, block_links, remainder)
    for step in range(MR_STEPS):
        dot_re = dot_im = norm = None
        for k in range(12):
            a_re, a_im, r_re, r_im = applied[k], applied[12 + k], remainder[k], remainder[12 + k]
            terms = (a_re * r_re + a_im * r_im, a_re * r_im - a_im * r_re, a_re * a_re + a_im * a_im)
            dot_re, dot_im, norm = terms if k == 0 else (dot_re + terms[0], dot_im + terms[1], norm + terms[2])
        norm = block_total(norm) + EPSILON
        alpha_re, alpha_im = block_total(dot_re) / norm, block_total(dot_im) / norm
        alpha_re = jnp.concatenate([alpha_re, alpha_re], axis=0)
        alpha_im = jnp.concatenate([alpha_im, alpha_im], axis=0)
        last = step == MR_STEPS - 1
        if not last:
            block_operator(again, clover, block_links, applied)
        for k in range(12):
            a_re, a_im, r_re, r_im = applied[k], applied[12 + k], remainder[k], remainder[12 + k]
            gain_re, gain_im = alpha_re * r_re - alpha_im * r_im, alpha_re * r_im + alpha_im * r_re
            correction[k] = gain_re if step == 0 else correction[k] + gain_re
            correction[12 + k] = gain_im if step == 0 else correction[12 + k] + gain_im
            remainder[k] = r_re - (alpha_re * a_re - alpha_im * a_im)
            remainder[12 + k] = r_im - (alpha_re * a_im + alpha_im * a_re)
            if not last:
                b_re, b_im = again[k], again[12 + k]
                applied[k] = a_re - (alpha_re * b_re - alpha_im * b_im)
                applied[12 + k] = a_im - (alpha_re * b_im + alpha_im * b_re)
    write_faces(sent, correction, links)
    for k in range(24):
        update[k] = start[k] + correction[k]


def inner_kernel(update, correction, remainder, links, update_hbm, latest, sem):
    copy = pltpu.make_async_copy(update, update_hbm, sem)
    copy.start()
    for k in range(24):
        latest[k] = remainder[k]
    ahead, behind = outside(3, 0.5)
    hop_terms(latest, links, correction, 3, ahead, behind, True)
    copy.wait()


def latest_kernel(partial, source_sq, links, *rest):
    received, sums, latest = rest[:6], rest[6], rest[7]
    for k in range(24):
        latest[k] = partial[k]
    halo_hops(latest, links, received)
    total = None
    for k in range(24):
        square = latest[k] * latest[k]
        total = square if total is None else total + square
    row = lax.broadcasted_iota(jnp.int32, (8, LANES), 0)
    lane = lax.broadcasted_iota(jnp.int32, (8, LANES), 1)
    summed = None
    for j, value in enumerate((total, source_sq[...])):
        for t in range(4):
            half = value[8 * (t // 2):8 * (t // 2) + 8]
            part = turned(over_rows(jnp.where(row // 4 == t % 2, half, 0.0)), 0, 1)
            summed = part if summed is None else jnp.where(lane % 8 == 4 * j + t, part, summed)
    summed = over_rows(summed)[:1]
    for k in range(sums.shape[0]):
        sums[k] = summed


def profile_kernel(gathered, profile):
    total = gathered[0]
    for k in range(1, gathered.shape[0]):
        total = total + gathered[k]
    total = jnp.broadcast_to(total, (8, LANES))
    residual = over_rows(turned(total, 0, 8) + turned(total, 64, 8))
    source = over_rows(turned(total, 4, 8) + turned(total, 68, 8))
    profile[...] = (residual / source)[:1, :4]


PARAMS = pltpu.CompilerParams(vmem_limit_bytes=12 * 2**20)
FIELD = pltpu.VMEM((24, ROWS, LANES), jnp.float32)
FACE = pltpu.VMEM((48, LANES), jnp.float32)
SCRATCH = pltpu.VMEM((24, ROWS, LANES), jnp.float32)
IN_HBM = pl.BlockSpec(memory_space=pltpu.HBM)
LINKS = pltpu.VMEM((72, ROWS, LANES), jnp.float32)


def in_vmem(value):
    return pltpu.with_memory_space_constraint(value, pltpu.VMEM)


def in_hbm(value):
    return pltpu.with_memory_space_constraint(value, pltpu.HBM)


def call(body, outs, scratch=(), flops=10_000_000):
    kernel = pl.pallas_call(
        body,
        out_shape=outs,
        scratch_shapes=scratch,
        compiler_params=PARAMS,
        cost_estimate=pl.CostEstimate(flops=flops, transcendentals=0, bytes_accessed=2_000_000),
    )
    return lambda *args: kernel(*map(in_vmem, args))


def matching(count, first):
    pairs = []
    for low in range(first, count + first, 2):
        a, b = low % count, (low + 1) % count
        pairs += [(a, b), (b, a)]
    return pairs


def exchange(faces):
    received = []
    for face, (direction, first) in zip(faces, MESSAGES):
        axis = AXES[direction]
        received.append(lax.ppermute(face, axis, matching(lax.axis_size(axis), first)))
    return received


def local(source, start_guess, gauge_links, clover):
    shape = source.shape
    source = source.reshape(24, ROWS, LANES)
    start = start_guess.reshape(24, ROWS, LANES)
    links = gauge_links.reshape(72, ROWS, LANES)
    clover = clover.reshape(144, ROWS, LANES)
    start, links, source, clover, *faces = pl.pallas_call(
        send_kernel,
        in_specs=[IN_HBM] * 4,
        out_shape=[FIELD, LINKS, FIELD, pltpu.VMEM((len(KEPT), ROWS, LANES), jnp.float32)]
        + [FACE] * 6,
        scratch_shapes=[pltpu.SemaphoreType.DMA((4 + len(clover_runs()),))],
        compiler_params=PARAMS,
    )(in_hbm(start), in_hbm(links), in_hbm(source), in_hbm(clover))
    received = exchange(faces)
    partial, source_sq, block_links = call(
        residual_kernel, [FIELD, pltpu.VMEM((ROWS, LANES), jnp.float32), LINKS])(source, start, links, clover)
    *faces, correction, remainder, update = call(sweep_kernel, [FACE] * 6 + [FIELD] * 3, [SCRATCH] * 2)(
        partial, start, links, block_links, clover, *received)
    received = exchange(faces)
    update, latest = call(
        inner_kernel, [pltpu.HBM(source.shape, jnp.float32), FIELD], [pltpu.SemaphoreType.DMA(())])(
            update, correction, remainder, links)
    group = GZ + ("gy",)
    sums = call(latest_kernel, pltpu.VMEM((lax.axis_size(group), 1, LANES), jnp.float32), [SCRATCH])(
        latest, source_sq, links, *received)
    sums = lax.all_to_all(sums, group, 0, 0)
    profile = call(profile_kernel, jax.ShapeDtypeStruct((1, 4), jnp.float32))(sums)
    return update.reshape(shape), profile.reshape(4)


def solution(mesh):
    finer = Mesh(
        mesh.devices.reshape(mesh.shape["ta"], 2, 2, mesh.shape["gy"]), ("ta", "gz_0", "gz_1", "gy")
    )
    field = P(None, None, None, "ta", GZ, "gy")
    matrix = P(None, None, None, None, "ta", GZ, "gy")
    return jax.shard_map(
        local, mesh=finer, in_specs=(field, field, matrix, matrix), out_specs=(field, P("ta")), check_vma=False
    )
```

```python
import jax
import jax.numpy as jnp
from jax import lax
from jax.experimental import pallas as pl
from jax.experimental.pallas import tpu as pltpu
from jax.sharding import Mesh
from jax.sharding import PartitionSpec as P

LX = 32
MR_STEPS = 4
EPSILON = 1e-06
GZ = ("gz_0", "gz_1")
ROWS, LANES = 16, 128
AXES = ("ta", GZ, "gy")
MESSAGES = ((0, 1), (0, 0), (2, 1), (2, 0), (1, 1), (1, 0))

UPPER = (
    ((0, 1), (1, 1)),
    ((0, -1j), (1, 1j)),
    ((1, -1), (0, 1)),
    ((1, -1j), (0, -1j)),
)


def plus(a, b):
    return a[0] + b[0], a[1] + b[1]


def plus_times(a, coef, b):
    if coef == 1:
        return a[0] + b[0], a[1] + b[1]
    if coef == -1:
        return a[0] - b[0], a[1] - b[1]
    if coef == 1j:
        return a[0] - b[1], a[1] + b[0]
    return a[0] + b[1], a[1] - b[0]


def iota(axis):
    return lax.broadcasted_iota(jnp.int32, (ROWS, LANES), axis)


def roll(value, shift, axis):
    size = value.shape[axis]
    shift = shift % size
    if shift == 0:
        return value
    return pltpu.roll(value, shift, axis)


def spinor_at(ref, spin, colour, rows=slice(None)):
    return ref[3 * spin + colour, rows], ref[12 + 3 * spin + colour, rows]


def half_spinor(ref, direction, row, sign, rows=slice(None)):
    column, entry = UPPER[direction][row]
    return [
        plus_times(spinor_at(ref, row, colour, rows), sign * entry, spinor_at(ref, 2 + column, colour, rows))
        for colour in range(3)
    ]


def link_at(links, direction, row, column, rows=slice(None)):
    base = 18 * direction + 3 * row + column
    return links[base, rows], links[base + 9, rows]


def link_times(links, direction, vector, rows=slice(None)):
    out = []
    for row in range(3):
        re = im = None
        for column in range(3):
            u_re, u_im = link_at(links, direction, row, column, rows)
            v_re, v_im = vector[column]
            t_re, t_im = u_re * v_re - u_im * v_im, u_re * v_im + u_im * v_re
            re, im = (t_re, t_im) if re is None else (re + t_re, im + t_im)
        out.append((re, im))
    return out


def link_adjoint_times(links, direction, vector, rows=slice(None)):
    out = []
    for row in range(3):
        re = im = None
        for column in range(3):
            u_re, u_im = link_at(links, direction, column, row, rows)
            v_re, v_im = vector[column]
            t_re, t_im = u_re * v_re + u_im * v_im, u_re * v_im - u_im * v_re
            re, im = (t_re, t_im) if re is None else (re + t_re, im + t_im)
        out.append((re, im))
    return out


def add_hops(out_ref, direction, row, forward, behind):
    column, entry = UPPER[direction][row]
    conj = complex(entry).conjugate()
    for colour in range(3):
        upper = plus(forward[colour], behind[colour])
        lower = plus_times(behind[colour], -1, forward[colour])
        for spin, coef, value in ((row, 1, upper), (2 + column, conj, lower)):
            k = 3 * spin + colour
            out_ref[k], out_ref[12 + k] = plus_times((out_ref[k], out_ref[12 + k]), coef, value)


def shift(value, direction, offset, periodic):
    if direction == 0:
        low, high = roll(value[:8], 4, 0), roll(value[8:], 4, 0)
        front = lax.broadcasted_iota(jnp.int32, (8, LANES), 0) < 4
        if offset > 0:
            return jnp.concatenate([jnp.where(front, low, high), high], axis=0)
        return jnp.concatenate([jnp.where(front, high, low), jnp.where(front, low, high)], axis=0)
    if direction == 1:
        return jnp.concatenate([roll(value[:8], -offset, 0), roll(value[8:], -offset, 0)], axis=0)
    if direction == 2:
        return roll(value, -LX * offset, 1)
    near = roll(value, -offset, 1)
    if not periodic:
        return near
    edge = (LX - 1) if offset > 0 else 0
    return jnp.where(iota(1) % LX == edge, roll(value, offset * (LX - 1), 1), near)


def inside(direction, offset):
    edge = 3 if offset > 0 else 0
    if direction == 0:
        return iota(0) // 4 != edge
    if direction == 1:
        return iota(0) % 4 != edge
    if direction == 2:
        return iota(1) // LX != edge
    return iota(1) % 4 != edge


def clover_runs():
    runs, kept = [], 0
    for chirality in range(2):
        for part in range(2):
            for a in range(6 - part):
                runs.append((72 * chirality + 36 * part + 7 * a + part, kept, 6 - part - a))
                kept += 6 - part - a
    return runs


KEPT = {first + k: kept + k for first, kept, rows in clover_runs() for k in range(rows)}


def site_terms(out_ref, clover, ref):
    for chirality in range(2):
        for a in range(6):
            re = im = None
            for b in range(6):
                place = 72 * chirality + 6 * min(a, b) + max(a, b)
                m_re = clover[KEPT[place]]
                v_re, v_im = ref[6 * chirality + b], ref[12 + 6 * chirality + b]
                t_re, t_im = m_re * v_re, m_re * v_im
                re, im = (t_re, t_im) if re is None else (re + t_re, im + t_im)
                if a != b:
                    m_im = clover[KEPT[place + 36]]
                    if a < b:
                        re, im = re - m_im * v_im, im + m_im * v_re
                    else:
                        re, im = re + m_im * v_im, im - m_im * v_re
            k = 6 * chirality + a
            out_ref[k] = re
            out_ref[12 + k] = im


def hop_terms(out_ref, links, ref, direction, ahead_weight=None, behind_weight=None, periodic=False):
    for row in range(2):
        ahead = half_spinor(ref, direction, row, -1)
        ahead = [tuple(shift(p, direction, 1, periodic) for p in c) for c in ahead]
        forward = link_times(links, direction, ahead)
        behind = link_adjoint_times(links, direction, half_spinor(ref, direction, row, 1))
        behind = [tuple(shift(p, direction, -1, periodic) for p in c) for c in behind]
        if ahead_weight is not None:
            forward = [tuple(p * ahead_weight for p in c) for c in forward]
            behind = [tuple(p * behind_weight for p in c) for c in behind]
        add_hops(out_ref, direction, row, forward, behind)


def outside(direction, scale):
    return [jnp.where(inside(direction, offset), jnp.float32(0.0), jnp.float32(scale)) for offset in (1, -1)]


def cut_links(block_links, links):
    for direction in range(4):
        weight = jnp.where(inside(direction, 1), jnp.float32(-0.5), jnp.float32(0.0))
        for k in range(18):
            block_links[18 * direction + k] = links[18 * direction + k] * weight


def block_operator(out_ref, clover, block_links, ref):
    site_terms(out_ref, clover, ref)
    for direction in range(4):
        hop_terms(out_ref, block_links, ref, direction)


def packed(vectors, direction, edge):
    flat = [part for vector in vectors for colour in vector for part in colour]
    tiles = []
    for group in range(3):
        tile = None
        for j in range(4):
            value = flat[4 * group + j]
            if direction == 0:
                moved, keep = roll(value, 4 * (j - edge), 0), iota(0) // 4 == j
            elif direction == 1:
                moved, keep = roll(value, j - edge, 0), iota(0) % 4 == j
            else:
                moved, keep = roll(value, LX * (j - edge), 1), iota(1) // LX == j
            tile = moved if tile is None else jnp.where(keep, moved, tile)
        tiles.append(tile)
    return tiles


def unpacked(tiles, direction, edge, scale):
    if direction == 0:
        weight = jnp.where(iota(0) // 4 == edge, scale, 0.0)
    elif direction == 1:
        weight = jnp.where(iota(0) % 4 == edge, scale, 0.0)
    else:
        weight = jnp.where(iota(1) // LX == edge, scale, 0.0)
    flat = []
    for group in range(3):
        for j in range(4):
            if direction == 0:
                moved = roll(tiles[group], 4 * (edge - j), 0)
            elif direction == 1:
                moved = roll(tiles[group], edge - j, 0)
            else:
                moved = roll(tiles[group], LX * (edge - j), 1)
            flat.append(moved * weight)
    pairs = [(flat[2 * k], flat[2 * k + 1]) for k in range(6)]
    return pairs[:3], pairs[3:]


def write_faces(face_refs, ref, links):
    for direction in range(3):
        up = packed(
            [link_adjoint_times(links, direction, half_spinor(ref, direction, row, 1)) for row in range(2)],
            direction, 3)
        down = packed([half_spinor(ref, direction, row, -1) for row in range(2)], direction, 0)
        even = lax.axis_index(AXES[direction]) % 2 == 0
        for group in range(3):
            rows = pl.ds(ROWS * group, ROWS)
            face_refs[MESSAGES.index((direction, 0))][rows] = jnp.where(even, up[group], down[group])
            face_refs[MESSAGES.index((direction, 1))][rows] = jnp.where(even, down[group], up[group])


def halo_hops(out_ref, links, face_refs):
    for direction in range(3):
        even = lax.axis_index(AXES[direction]) % 2 == 0
        above, below = [], []
        for group in range(3):
            rows = pl.ds(ROWS * group, ROWS)
            first, second = (face_refs[MESSAGES.index((direction, k))][rows] for k in range(2))
            above.append(jnp.where(even, first, second))
            below.append(jnp.where(even, second, first))
        scale_above = scale_below = jnp.float32(0.5)
        if direction == 0:
            place, last = lax.axis_index("ta"), lax.axis_size("ta") - 1
            scale_above = jnp.where(place == last, jnp.float32(-0.5), jnp.float32(0.5))
            scale_below = jnp.where(place == 0, jnp.float32(-0.5), jnp.float32(0.5))
        ahead = unpacked(above, direction, 3, scale_above)
        behind = unpacked(below, direction, 0, scale_below)
        for row in range(2):
            add_hops(out_ref, direction, row, link_times(links, direction, ahead[row]), behind[row])


def over_rows(value):
    for step in (4, 2, 1):
        value = value + roll(value, step, 0)
    return value


def turned(value, shift, stride):
    return pltpu.roll(value, shift, 1, stride=stride, stride_axis=0)


def block_total(value):
    total = over_rows(value[:8] + value[8:])
    row = lax.broadcasted_iota(jnp.int32, (8, LANES), 0)
    place = lax.broadcasted_iota(jnp.int32, (8, LANES), 1) % 4
    spread = None
    for shift, last in ((LX - 3, 7), (2 * LX - 3, 7), (3 * LX - 3, 7), (0, 7), (LANES - 7, 6)):
        source = place - (row + ((shift + 16) % LX - 16))
        part = jnp.where((source >= 0) & (source < 4) & (row <= last), turned(total, shift, 1), 0.0)
        spread = part if spread is None else spread + part
    return over_rows(spread)


def send_kernel(start_hbm, links_hbm, clover_hbm, start, links, clover, *rest):
    faces, sems = rest[:6], rest[6]
    near, far = pl.ds(0, 54), pl.ds(54, 18)
    copies = [
        pltpu.make_async_copy(start_hbm, start, sems.at[0]),
        pltpu.make_async_copy(links_hbm.at[near], links.at[near], sems.at[1]),
        pltpu.make_async_copy(links_hbm.at[far], links.at[far], sems.at[2]),
    ]
    for k, (first, kept, rows) in enumerate(clover_runs()):
        copies.append(
            pltpu.make_async_copy(clover_hbm.at[pl.ds(first, rows)], clover.at[pl.ds(kept, rows)], sems.at[3 + k]))
    for copy in copies:
        copy.start()
    copies[0].wait()
    copies[1].wait()
    write_faces(faces, start, links)
    for copy in copies[2:]:
        copy.wait()


def residual_kernel(source_hbm, start, links, clover, partial, source_sq, block_links, source, sem):
    copy = pltpu.make_async_copy(source_hbm, source, sem)
    copy.start()
    cut_links(block_links, links)
    site_terms(partial, clover, start)
    for direction in range(3):
        hop_terms(partial, block_links, start, direction)
    half = jnp.float32(-0.5)
    hop_terms(partial, links, start, 3, half, half, True)
    copy.wait()
    total = None
    for k in range(24):
        value = source[k]
        partial[k] = value - partial[k]
        total = value * value if total is None else total + value * value
    source_sq[...] = total


def sweep_kernel(partial, start, links, block_links, clover, *rest):
    received, sent = rest[:6], rest[6:12]
    correction, remainder, update, applied, again = rest[12:]
    for k in range(24):
        remainder[k] = partial[k]
    halo_hops(remainder, links, received)
    block_operator(applied, clover, block_links, remainder)
    for step in range(MR_STEPS):
        dot_re = dot_im = norm = None
        for k in range(12):
            a_re, a_im, r_re, r_im = applied[k], applied[12 + k], remainder[k], remainder[12 + k]
            terms = (a_re * r_re + a_im * r_im, a_re * r_im - a_im * r_re, a_re * a_re + a_im * a_im)
            dot_re, dot_im, norm = terms if k == 0 else (dot_re + terms[0], dot_im + terms[1], norm + terms[2])
        norm = block_total(norm) + EPSILON
        alpha_re, alpha_im = block_total(dot_re) / norm, block_total(dot_im) / norm
        alpha_re = jnp.concatenate([alpha_re, alpha_re], axis=0)
        alpha_im = jnp.concatenate([alpha_im, alpha_im], axis=0)
        last = step == MR_STEPS - 1
        if not last:
            block_operator(again, clover, block_links, applied)
        for k in range(12):
            a_re, a_im, r_re, r_im = applied[k], applied[12 + k], remainder[k], remainder[12 + k]
            gain_re, gain_im = alpha_re * r_re - alpha_im * r_im, alpha_re * r_im + alpha_im * r_re
            correction[k] = gain_re if step == 0 else correction[k] + gain_re
            correction[12 + k] = gain_im if step == 0 else correction[12 + k] + gain_im
            remainder[k] = r_re - (alpha_re * a_re - alpha_im * a_im)
            remainder[12 + k] = r_im - (alpha_re * a_im + alpha_im * a_re)
            if not last:
                b_re, b_im = again[k], again[12 + k]
                applied[k] = a_re - (alpha_re * b_re - alpha_im * b_im)
                applied[12 + k] = a_im - (alpha_re * b_im + alpha_im * b_re)
    write_faces(sent, correction, links)
    for k in range(24):
        update[k] = start[k] + correction[k]


def inner_kernel(update, correction, remainder, links, update_hbm, latest, sem):
    copy = pltpu.make_async_copy(update, update_hbm, sem)
    copy.start()
    for k in range(24):
        latest[k] = remainder[k]
    ahead, behind = outside(3, 0.5)
    hop_terms(latest, links, correction, 3, ahead, behind, True)
    copy.wait()


def latest_kernel(partial, source_sq, links, *rest):
    received, sums, latest = rest[:6], rest[6], rest[7]
    for k in range(24):
        latest[k] = partial[k]
    halo_hops(latest, links, received)
    total = None
    for k in range(24):
        square = latest[k] * latest[k]
        total = square if total is None else total + square
    row = lax.broadcasted_iota(jnp.int32, (8, LANES), 0)
    lane = lax.broadcasted_iota(jnp.int32, (8, LANES), 1)
    summed = None
    for j, value in enumerate((total, source_sq[...])):
        for t in range(4):
            half = value[8 * (t // 2):8 * (t // 2) + 8]
            part = turned(over_rows(jnp.where(row // 4 == t % 2, half, 0.0)), 0, 1)
            summed = part if summed is None else jnp.where(lane % 8 == 4 * j + t, part, summed)
    summed = over_rows(summed)[:1]
    for k in range(sums.shape[0]):
        sums[k] = summed


def profile_kernel(gathered, profile):
    total = gathered[0]
    for k in range(1, gathered.shape[0]):
        total = total + gathered[k]
    total = jnp.broadcast_to(total, (8, LANES))
    residual = over_rows(turned(total, 0, 8) + turned(total, 64, 8))
    source = over_rows(turned(total, 4, 8) + turned(total, 68, 8))
    profile[...] = (residual / source)[:1, :4]


PARAMS = pltpu.CompilerParams(vmem_limit_bytes=12 * 2**20)
FIELD = pltpu.VMEM((24, ROWS, LANES), jnp.float32)
FACE = pltpu.VMEM((48, LANES), jnp.float32)
SCRATCH = pltpu.VMEM((24, ROWS, LANES), jnp.float32)
IN_HBM = pl.BlockSpec(memory_space=pltpu.HBM)
LINKS = pltpu.VMEM((72, ROWS, LANES), jnp.float32)


def in_vmem(value):
    return pltpu.with_memory_space_constraint(value, pltpu.VMEM)


def in_hbm(value):
    return pltpu.with_memory_space_constraint(value, pltpu.HBM)


def call(body, outs, scratch=(), flops=10_000_000):
    kernel = pl.pallas_call(
        body,
        out_shape=outs,
        scratch_shapes=scratch,
        compiler_params=PARAMS,
        cost_estimate=pl.CostEstimate(flops=flops, transcendentals=0, bytes_accessed=2_000_000),
    )
    return lambda *args: kernel(*map(in_vmem, args))


def matching(count, first):
    pairs = []
    for low in range(first, count + first, 2):
        a, b = low % count, (low + 1) % count
        pairs += [(a, b), (b, a)]
    return pairs


def exchange(faces):
    received = []
    for face, (direction, first) in zip(faces, MESSAGES):
        axis = AXES[direction]
        received.append(lax.ppermute(face, axis, matching(lax.axis_size(axis), first)))
    return received


def local(source, start_guess, gauge_links, clover):
    shape = source.shape
    source = source.reshape(24, ROWS, LANES)
    start = start_guess.reshape(24, ROWS, LANES)
    links = gauge_links.reshape(72, ROWS, LANES)
    clover = clover.reshape(144, ROWS, LANES)
    start, links, clover, *faces = pl.pallas_call(
        send_kernel,
        in_specs=[IN_HBM] * 3,
        out_shape=[FIELD, LINKS, pltpu.VMEM((len(KEPT), ROWS, LANES), jnp.float32)] + [FACE] * 6,
        scratch_shapes=[pltpu.SemaphoreType.DMA((3 + len(clover_runs()),))],
        compiler_params=PARAMS,
    )(in_hbm(start), in_hbm(links), in_hbm(clover))
    received = exchange(faces)
    partial, source_sq, block_links = pl.pallas_call(
        residual_kernel,
        in_specs=[IN_HBM] + [pl.BlockSpec(memory_space=pltpu.VMEM)] * 3,
        out_shape=[FIELD, pltpu.VMEM((ROWS, LANES), jnp.float32), LINKS],
        scratch_shapes=[SCRATCH, pltpu.SemaphoreType.DMA(())],
        compiler_params=PARAMS,
        cost_estimate=pl.CostEstimate(flops=10_000_000, transcendentals=0, bytes_accessed=2_000_000),
    )(in_hbm(source), *map(in_vmem, (start, links, clover)))
    *faces, correction, remainder, update = call(sweep_kernel, [FACE] * 6 + [FIELD] * 3, [SCRATCH] * 2)(
        partial, start, links, block_links, clover, *received)
    received = exchange(faces)
    update, latest = call(
        inner_kernel, [pltpu.HBM(source.shape, jnp.float32), FIELD], [pltpu.SemaphoreType.DMA(())])(
            update, correction, remainder, links)
    group = GZ + ("gy",)
    sums = call(latest_kernel, pltpu.VMEM((lax.axis_size(group), 1, LANES), jnp.float32), [SCRATCH])(
        latest, source_sq, links, *received)
    sums = lax.all_to_all(sums, group, 0, 0)
    profile = call(profile_kernel, jax.ShapeDtypeStruct((1, 4), jnp.float32))(sums)
    return update.reshape(shape), profile.reshape(4)


def solution(mesh):
    finer = Mesh(
        mesh.devices.reshape(mesh.shape["ta"], 2, 2, mesh.shape["gy"]), ("ta", "gz_0", "gz_1", "gy")
    )
    field = P(None, None, None, "ta", GZ, "gy")
    matrix = P(None, None, None, None, "ta", GZ, "gy")
    return jax.shard_map(
        local, mesh=finer, in_specs=(field, field, matrix, matrix), out_specs=(field, P("ta")), check_vma=False
    )
```
